256 devices in a mesh: samp: 8 (over x, core), snp: 32 (over y, z).
Axes of the slice: x: 4, y: 4, z: 8, core: 2. Of those that a mesh axis runs over, the one named last changes fastest.
Arguments:
- genotype: bfloat16 [40960, 40960], P('samp', 'snp'), may hold values from 0 to 2, as said below
- centre: float32 [40960], P('snp'), may hold values from 0.1 to 1
- spread: float32 [40960], P('snp'), may hold values from 0.308 to 0.7072
- pheno_probes: float32 [32, 40960], P(None, ('samp', 'snp')), may hold values from -15.75 to 15.75
Outputs:
- solution: float32 [32, 40960], P(None, ('samp', 'snp'))
- marker_stats: float32 [32, 40960], P(None, 'snp')
The draws below stay inside these ranges and needn't reach their ends.
Inputs may be any that keep to these rules, and one draw needn't show every extreme that they name: `genotype`: whole numbers.
All inputs are finite; a program needn't handle non-finite values.
Results may differ from the reference program's by a relative error of at most 0.0003.
Values sent between devices are 32-bit elements; how exact they have to be, the bound alone decides.
A program may use at most 128 MiB of HBM per device.

```python
import math
import jax
import jax.numpy as jnp
from jax import lax

SAMPLES = 40960
MARKERS = 40960
PROBES = 32
ROUNDS = 3
N_SNP = 32


def allele_rate(key):
    return jax.random.randint(jax.random.fold_in(key, 11), (MARKERS,), 50, 501)


def draw_genotype(key, part):
    rates = allele_rate(key)
    coded = jax.random.randint(jax.random.fold_in(key, 23), (SAMPLES, MARKERS), 0, 1000000)
    leading_replica = (coded % 1000 < rates[None, :]).astype(jnp.int32)
    second_copy = (coded // 1000 < rates[None, :]).astype(jnp.int32)
    return (leading_replica + second_copy).astype(jnp.float32).astype(jnp.bfloat16)


def draw_centre(key, part):
    rates = allele_rate(key).astype(jnp.float32) / 1000.0
    return 2.0 * rates


def draw_spread(key, part):
    rates = allele_rate(key).astype(jnp.float32) / 1000.0
    return jnp.sqrt(2.0 * rates * (1.0 - rates))


def draw_pheno_probes(key, part):
    position = jnp.arange(SAMPLES, dtype=jnp.float32) / (SAMPLES - 1)
    noise = jnp.clip(jax.random.normal(jax.random.fold_in(key, 31), (PROBES, SAMPLES), jnp.float32), -4.0, 4.0)
    return noise * (1.0 + 2.0 * position)[None, :]


def setup_inputs(seed: int = 0) -> dict:
    arg_keys = jax.random.split(jax.random.key(seed), 5)
    genotype = draw_genotype(jax.random.fold_in(arg_keys[4], 71), 0)
    centre = draw_centre(jax.random.fold_in(arg_keys[4], 71), 0)
    spread = draw_spread(jax.random.fold_in(arg_keys[4], 71), 0)
    pheno_probes = draw_pheno_probes(jax.random.fold_in(arg_keys[4], 71), 0)
    return {"genotype": genotype, "centre": centre, "spread": spread, "pheno_probes": pheno_probes}


ridge = 0.1
exact = lax.Precision.HIGHEST

def block_scores(genotype, centre, spread, first, width):
    columns = lax.dynamic_slice_in_dim(genotype, first, width, 1)
    middles = lax.dynamic_slice_in_dim(centre, first, width, 0)
    deviations = lax.dynamic_slice_in_dim(spread, first, width, 0)
    return (columns.astype(jnp.float32) - middles[None, :]) / deviations[None, :]

def operate(vector, genotype, centre, spread):
    width = MARKERS // N_SNP

    def add_block(index, running):
        first = (index * width).astype(jnp.int32)
        scores = block_scores(genotype, centre, spread, first, width)
        marker_load = jnp.dot(vector, scores, precision=exact, preferred_element_type=jnp.float32)
        return running + lax.dot_general(marker_load, scores, (((1,), (1,)), ((), ())), precision=exact, preferred_element_type=jnp.float32)
    summed = lax.fori_loop(jnp.int32(0), jnp.int32(N_SNP), add_block, jnp.zeros(vector.shape, jnp.float32))
    return summed / MARKERS + ridge * vector

def association(solution, genotype, centre, spread):
    width = MARKERS // N_SNP

    def one_block(index, running):
        first = (index * width).astype(jnp.int32)
        scores = block_scores(genotype, centre, spread, first, width)
        marker_load = jnp.dot(solution, scores, precision=exact, preferred_element_type=jnp.float32)
        return lax.dynamic_update_slice_in_dim(running, marker_load, first, 1)
    gathered = lax.fori_loop(jnp.int32(0), jnp.int32(N_SNP), one_block, jnp.zeros((PROBES, MARKERS), jnp.float32))
    return gathered / math.sqrt(SAMPLES)

def reference(genotype, centre, spread, pheno_probes):
    solution = jnp.zeros_like(pheno_probes)
    residual = pheno_probes
    direction = pheno_probes
    norm_now = lax.optimization_barrier(jnp.sum(residual * residual, axis=1, keepdims=True))
    for counter in range(ROUNDS):
        applied = operate(direction, genotype, centre, spread)
        step_size = norm_now / lax.optimization_barrier(jnp.sum(direction * applied, axis=1, keepdims=True))
        solution = solution + step_size * direction
        residual = residual - step_size * applied
        norm_next = lax.optimization_barrier(jnp.sum(residual * residual, axis=1, keepdims=True))
        direction = residual + norm_next / norm_now * direction
        norm_now = norm_next
    return (solution, association(solution, genotype, centre, spread))
```

```python
import math

import jax
import jax.numpy as jnp
from jax import lax
from jax.experimental import pallas as pl
from jax.experimental.pallas import tpu as pltpu
from jax.sharding import PartitionSpec as P

SAMPLES = 40960
MARKERS = 40960
ROUNDS = 3
RIDGE = 0.1

ROWS = 32
NY, NZ = 4, 8
NX = 4
PEERS = NY * NZ
CHUNK = 640
BLOCK = CHUNK * NZ
COLS = 1280
WIDE = COLS + 128
PIECE = 8 * CHUNK

MESH = pl.DeviceIdType.MESH
NEAR = (1, 7, 2, 6, 3, 5, 4)
f32 = jnp.float32


def near(step):
    half = (step + 1) // 2
    return jnp.where(step % 2 == 1, half, (NZ - half) % NZ)


def split(value):
    high = value.astype(jnp.bfloat16)
    rest = value - high.astype(f32)
    return high, rest.astype(jnp.bfloat16)


def lanes_summed(value):
    total = value[:, 0:128]
    for tile in range(1, value.shape[1] // 128):
        total = total + value[:, 128 * tile : 128 * (tile + 1)]
    return total


def kernel(
    geno_hbm, rhs_ref, centre_ref, spread_ref, solution_ref, stats_ref,
    geno, r_0, r_1, r_2, packed, u_0, u_1, from_y_0, from_y_1, to_z_0, to_z_1,
    from_z_0, from_z_1, partial, acc, loads_out, from_core, by_x, loads_in,
    scalars, lhs, dir_loads, steps, betas,
    geno_sem, s_gz, s_gy, s_ry, s_rz, s_core, s_x, s_back, s_sc,
    gz, gy, ry, rz, core_sem, x_sem, back_sem, sc_sem,
):
    samp, snp = lax.axis_index("samp"), lax.axis_index("snp")
    x, core = samp // 2, samp % 2
    y, z = snp // NZ, snp % NZ
    residuals = (r_0, r_1, r_2)

    def at_z(other):
        return (samp, y * NZ + other)

    def at_y(other):
        return (samp, other * NZ + z)

    def at_x(other):
        return (other * 2 + core, snp)

    partner = (x * 2 + 1 - core, snp)

    def send(source, target, send_sem, recv_sem, device):
        pltpu.make_async_remote_copy(
            source, target, send_sem, recv_sem, device_id=device, device_id_type=MESH
        ).start()

    def settle(sem, like):
        pltpu.make_async_copy(like, like, sem).wait()

    pieces = r_0.at[0:24, 0:CHUNK]

    def rows_of(group):
        return pl.ds(pl.multiple_of(group * 8, 8), 8)

    def cols_of(chunk):
        return pl.ds(pl.multiple_of(chunk * CHUNK, 128), CHUNK)

    for zz in range(NZ):
        for yy in range(NY):
            first = 160 * (yy * NZ + zz)
            pltpu.make_async_copy(
                geno_hbm.at[pl.ds(first, 128)], geno.at[pl.ds(CHUNK * zz + 128 * yy, 128)], geno_sem
            ).start()
            pltpu.make_async_copy(
                geno_hbm.at[pl.ds(first + 128, 32)],
                geno.at[pl.ds(CHUNK * zz + 512 + 32 * yy, 32)],
                geno_sem,
            ).start()

    barrier = pltpu.get_barrier_semaphore()

    def greet(offset, carry):
        pl.semaphore_signal(
            barrier, inc=1, device_id=(samp, (snp + offset) % PEERS), device_id_type=MESH
        )
        return carry

    lax.fori_loop(1, PEERS, greet, 0)
    pl.semaphore_signal(barrier, inc=1, device_id=partner, device_id_type=MESH)
    for dx in range(1, NX):
        pl.semaphore_signal(barrier, inc=1, device_id=at_x((x + dx) % NX), device_id_type=MESH)

    def main_cols(zz):
        return pl.ds(pl.multiple_of(zz * CHUNK + y * 128, 128), 128)

    r_0[:, main_cols(z)] = rhs_ref[:, 0:128]
    tails = [rhs_ref[8 * group : 8 * group + 8, 128:160] for group in range(4)]
    packed[y, z] = jnp.concatenate(tails, axis=1)
    pl.semaphore_wait(barrier, PEERS - 1 + NX)

    def forward_own(k, zz):
        for dy in range(1, NY):
            other = at_y((y + dy) % NY)
            if k == 0:
                block = r_0.at[:, main_cols(zz)]
                send(block, block, s_gy.at[0], gy.at[0, zz], other)
                send(packed.at[y, zz], packed.at[y, zz], s_gy.at[0], gy.at[0, zz], other)
            else:
                block = residuals[k].at[rows_of(y), cols_of(zz)]
                send(block, block, s_gy.at[k], gy.at[k, zz], other)

    def gather(k):
        for d in NEAR:
            other = at_z((z + d) % NZ)
            if k == 0:
                block = r_0.at[:, main_cols(z)]
                send(block, block, s_gz.at[0], gz.at[0, d - 1], other)
                send(packed.at[y, z], packed.at[y, z], s_gz.at[0], gz.at[0, d - 1], other)
            else:
                block = residuals[k].at[rows_of(y), cols_of(z)]
                send(block, block, s_gz.at[k], gz.at[k, d - 1], other)
        forward_own(k, z)
        for d in NEAR:
            settle(gz.at[k, d - 1], r_0.at[0:8, 0:CHUNK])
            forward_own(k, (z - d + NZ) % NZ)

    lane = lax.broadcasted_iota(jnp.int32, (8, 128), 1)

    def unpack(zz):
        sources = [packed[yy, zz] for yy in range(NY)]
        for group in range(4):
            tile = jnp.zeros((8, 128), f32)
            for yy in range(NY):
                shift = (32 * (yy - group)) % 128
                moved = pltpu.roll(sources[yy], shift, 1) if shift else sources[yy]
                tile = jnp.where(lane // 32 == yy, moved, tile)
            start = pl.multiple_of(zz * CHUNK + 512, 128)
            r_0[8 * group : 8 * group + 8, pl.ds(start, 128)] = tile

    def to_loads(k):
        partial[...] = jnp.zeros_like(partial)
        acc[...] = jnp.zeros_like(acc)

        def chunk(step, carry):
            zz = (z - near(step) + NZ) % NZ
            settle(gy.at[k, zz], pieces)
            if k == 0:
                unpack(zz)
            value = residuals[k][:, cols_of(zz)]
            high, low = split(value)
            partial[...] += jnp.dot(
                jnp.concatenate([high, low], axis=0),
                geno[cols_of(zz), :],
                preferred_element_type=f32,
            )
            acc[0] += lanes_summed(high.astype(f32) + low.astype(f32))
            acc[1] += lanes_summed(value * value)
            if k > 0:
                acc[2] += lanes_summed(value * residuals[k - 1][:, cols_of(zz)])
            if k > 1:
                acc[3] += lanes_summed(value * r_0[:, cols_of(zz)])
            return carry

        lax.fori_loop(0, NZ, chunk, 0)

    lane32 = lax.broadcasted_iota(jnp.int32, (ROWS, 128), 1)
    eye = lax.broadcasted_iota(jnp.int32, (ROWS, 128), 0) == lane32

    def over_samp(k):
        out, got, halves, full = loads_out.at[k], from_core.at[k], by_x.at[k], loads_in.at[k]
        total = jnp.sum(acc[0], axis=1, keepdims=True)
        raw = partial[0:ROWS] + partial[ROWS : 2 * ROWS]
        out[:, 0:COLS] = (raw - total * centre_ref[...]) / spread_ref[...]
        tile = jnp.zeros((ROWS, 128), f32)
        for which in range(1, 2 + k):
            tile = jnp.where(lane32 == which - 1, jnp.sum(acc[which], axis=1, keepdims=True), tile)
        out[:, COLS:WIDE] = tile
        mine = pl.ds(pl.multiple_of(core * 16, 16), 16)
        theirs = pl.ds(pl.multiple_of(16 - core * 16, 16), 16)
        send(out.at[theirs], got, s_core.at[k], core_sem.at[k], partner)
        settle(core_sem.at[k], got)
        halves[x] = out[mine, :] + got[...]
        for dx in (2, 1, 3):
            send(halves.at[x], halves.at[x], s_x.at[k], x_sem.at[k], at_x((x + dx) % NX))
        settle(x_sem.at[k], halves.at[0:3])
        full[mine, :] = (halves[0] + halves[1]) + (halves[2] + halves[3])
        send(full.at[mine], full.at[mine], s_back.at[k], back_sem.at[k], partner)
        settle(back_sem.at[k], full.at[mine])

    def spread_norms(k):
        loads = dir_loads[...]
        norm = jnp.sum(lanes_summed(loads * loads), axis=1, keepdims=True)
        row = jnp.sum(jnp.where(eye, norm, 0.0), axis=0, keepdims=True)
        scalars[k, snp] = row

        def one(offset, carry):
            slot = scalars.at[k, snp]
            send(slot, slot, s_sc.at[k], sc_sem.at[k], (samp, (snp + offset) % PEERS))
            return carry

        lax.fori_loop(1, PEERS, one, 0)

    def total_norms(k):
        settle(sc_sem.at[k], scalars.at[k, 0 : PEERS - 1])
        row = jnp.sum(scalars[k], axis=0)
        return jnp.sum(jnp.where(eye, row, 0.0), axis=1, keepdims=True)

    def to_image(k):
        image, from_y, to_z, from_z = (
            (u_0, from_y_0, to_z_0, from_z_0), (u_1, from_y_1, to_z_1, from_z_1)
        )[k]
        high, low = split(dir_loads[...] / spread_ref[...])
        lhs[0:ROWS] = high
        lhs[ROWS : 2 * ROWS] = low
        shift = (high.astype(f32) + low.astype(f32)) * centre_ref[...]
        shift = jnp.sum(lanes_summed(shift), axis=1, keepdims=True)

        def chunk(step, carry):
            zz = (z + near(NZ - 1 - step)) % NZ
            both = lax.dot_general(
                lhs[...], geno[cols_of(zz), :], (((1,), (1,)), ((), ())),
                preferred_element_type=f32,
            )
            image[:, cols_of(zz)] = both[0:ROWS] + both[ROWS : 2 * ROWS] - shift
            for dy in range(1, NY):
                other = (y + dy) % NY
                send(
                    image.at[rows_of(other), cols_of(zz)], from_y.at[dy - 1, :, cols_of(zz)],
                    s_ry.at[k], ry.at[k, zz], at_y(other),
                )
            return carry

        lax.fori_loop(0, NZ, chunk, 0)

        def pass_on(step, carry):
            offset = near(NZ - 1 - step)
            zz = (z + offset) % NZ
            settle(ry.at[k, zz], pieces)
            total = image[rows_of(y), cols_of(zz)]
            for dy in range(NY - 1):
                total = total + from_y[dy, :, cols_of(zz)]
            to_z[zz] = total

            @pl.when(step < NZ - 1)
            def _():
                send(to_z.at[zz], from_z.at[offset - 1], s_rz.at[k], rz.at[k], at_z(zz))

            return carry

        lax.fori_loop(0, NZ, pass_on, 0)
        settle(rz.at[k], from_z)
        total = to_z[z]
        for d in range(NZ - 1):
            total = total + from_z[d]
        return total

    norms, squares = [], []
    for k in range(ROUNDS):
        gather(k)
        if k == 0:
            settle(geno_sem, geno)
        to_loads(k)
        over_samp(k)
        loads = loads_in[k, :, 0:COLS]
        norm = loads_in[k, :, COLS : COLS + 1]
        if k == 0:
            dir_loads[...] = loads
            square = norm
        else:
            beta = norm / norms[-1]
            dir_loads[...] = loads + beta * dir_loads[...]
            cross = loads_in[k, :, COLS + 1 : COLS + 2]
            if k == 2:
                cross = cross + betas[0][:, 0:1] * loads_in[k, :, COLS + 2 : COLS + 3]
            square = norm + 2.0 * beta * cross + beta * beta * squares[-1]
            betas[k - 1] = jnp.broadcast_to(beta, (ROWS, 128))
        norms.append(norm)
        squares.append(square)
        spread_norms(k)
        if k < ROUNDS - 1:
            summed = to_image(k)
        size = norm / (total_norms(k) * (1.0 / MARKERS) + RIDGE * square)
        steps[k] = jnp.broadcast_to(size, (ROWS, 128))
        gain = size * (1.0 / math.sqrt(SAMPLES))
        if k == 0:
            stats_ref[...] = gain * dir_loads[...]
        else:
            stats_ref[...] += gain * dir_loads[...]
        if k < ROUNDS - 1:
            mine = (rows_of(y), cols_of(z))
            direction = residuals[k][mine]
            if k == 1:
                direction = direction + betas[0, rows_of(y), 0:1] * r_0[mine]
            moved = summed * (1.0 / MARKERS) + RIDGE * direction
            residuals[k + 1][mine] = residuals[k][mine] - steps[k, rows_of(y), 0:1] * moved

    def combined(columns):
        first = r_0[:, columns]
        second = r_1[:, columns] + betas[0][:, 0:1] * first
        third = r_2[:, columns] + betas[1][:, 0:1] * second
        return steps[0][:, 0:1] * first + steps[1][:, 0:1] * second + steps[2][:, 0:1] * third

    solution_ref[:, 0:128] = combined(main_cols(z))
    tail = combined(pl.ds(pl.multiple_of(z * CHUNK + 512, 128), 128))
    for yy in range(NY):

        @pl.when(y == yy)
        def _():
            solution_ref[:, 128:160] = tail[:, 32 * yy : 32 * yy + 32]

    for k in range(ROUNDS):
        settle(s_gz.at[k], from_z_0)
        settle(s_gy.at[k], r_0.at[0:24])
        settle(s_core.at[k], from_core.at[k])
        settle(s_x.at[k], by_x.at[k, 0:3])
        settle(s_back.at[k], from_core.at[k])
        settle(s_sc.at[k], scalars.at[k, 0 : PEERS - 1])
    for k in range(ROUNDS - 1):
        settle(s_ry.at[k], r_0.at[0:24])
        settle(s_rz.at[k], from_z_0)


def local(genotype, centre, spread, pheno_probes):
    block = (ROWS, BLOCK)
    dma = pltpu.SemaphoreType.DMA
    vmem = pl.BlockSpec(memory_space=pltpu.VMEM)
    return pl.pallas_call(
        kernel,
        out_shape=(
            jax.ShapeDtypeStruct((ROWS, 160), f32),
            jax.ShapeDtypeStruct((ROWS, COLS), f32),
        ),
        in_specs=[pl.BlockSpec(memory_space=pl.ANY), vmem, vmem, vmem],
        out_specs=(vmem, vmem),
        scratch_shapes=[
            pltpu.VMEM((BLOCK, COLS), jnp.bfloat16),
            pltpu.VMEM(block, f32),
            pltpu.VMEM(block, f32),
            pltpu.VMEM(block, f32),
            pltpu.VMEM((NY, NZ, 8, 128), f32),
            pltpu.VMEM(block, f32),
            pltpu.VMEM(block, f32),
            pltpu.VMEM((NY - 1, 8, BLOCK), f32),
            pltpu.VMEM((NY - 1, 8, BLOCK), f32),
            pltpu.VMEM((NZ, 8, CHUNK), f32),
            pltpu.VMEM((NZ, 8, CHUNK), f32),
            pltpu.VMEM((NZ - 1, 8, CHUNK), f32),
            pltpu.VMEM((NZ - 1, 8, CHUNK), f32),
            pltpu.VMEM((2 * ROWS, COLS), f32),
            pltpu.VMEM((4, ROWS, 128), f32),
            pltpu.VMEM((ROUNDS, ROWS, WIDE), f32),
            pltpu.VMEM((ROUNDS, 16, WIDE), f32),
            pltpu.VMEM((ROUNDS, NX, 16, WIDE), f32),
            pltpu.VMEM((ROUNDS, ROWS, WIDE), f32),
            pltpu.VMEM((ROUNDS, PEERS, 1, 128), f32),
            pltpu.VMEM((2 * ROWS, COLS), jnp.bfloat16),
            pltpu.VMEM((ROWS, COLS), f32),
            pltpu.VMEM((ROUNDS, ROWS, 128), f32),
            pltpu.VMEM((ROUNDS - 1, ROWS, 128), f32),
            dma,
            dma((ROUNDS,)),
            dma((ROUNDS,)),
            dma((ROUNDS - 1,)),
            dma((ROUNDS - 1,)),
            dma((ROUNDS,)),
            dma((ROUNDS,)),
            dma((ROUNDS,)),
            dma((ROUNDS,)),
            dma((ROUNDS, NZ - 1)),
            dma((ROUNDS, NZ)),
            dma((ROUNDS - 1, NZ)),
            dma((ROUNDS - 1,)),
            dma((ROUNDS,)),
            dma((ROUNDS,)),
            dma((ROUNDS,)),
            dma((ROUNDS,)),
        ],
        compiler_params=pltpu.CompilerParams(
            collective_id=0, has_side_effects=True, vmem_limit_bytes=48 * 1024 * 1024
        ),
        name="conjugate_gradients",
    )(genotype, pheno_probes, centre.reshape(1, COLS), spread.reshape(1, COLS))


def solution(mesh):
    in_specs = (P("samp", "snp"), P("snp"), P("snp"), P(None, ("samp", "snp")))
    out_specs = (P(None, ("samp", "snp")), P(None, "snp"))
    return jax.shard_map(local, mesh=mesh, in_specs=in_specs, out_specs=out_specs, check_vma=False)
```

```python
import math

import jax
import jax.numpy as jnp
from jax import lax
from jax.experimental import pallas as pl
from jax.experimental.pallas import tpu as pltpu
from jax.sharding import PartitionSpec as P

SAMPLES = 40960
MARKERS = 40960
ROUNDS = 3
RIDGE = 0.1

ROWS = 32
NY, NZ = 4, 8
NX = 4
PEERS = NY * NZ
CHUNK = 640
BLOCK = CHUNK * NZ
COLS = 1280
WIDE = COLS + 128
PIECE = 8 * CHUNK

MESH = pl.DeviceIdType.MESH
FAR = (2, 6, 3, 5, 4)
SCATTER = (4, 3, 5, 1, 7, 2, 6, 0)
f32 = jnp.float32


def near(step):
    half = (step + 1) // 2
    return jnp.where(step % 2 == 1, half, (NZ - half) % NZ)


def scatter_order(step):
    offset = jnp.int32(SCATTER[0])
    for place in range(1, NZ):
        offset = jnp.where(step == place, SCATTER[place], offset)
    return offset


def split(value):
    high = value.astype(jnp.bfloat16)
    rest = value - high.astype(f32)
    return high, rest.astype(jnp.bfloat16)


def lanes_summed(value):
    total = value[:, 0:128]
    for tile in range(1, value.shape[1] // 128):
        total = total + value[:, 128 * tile : 128 * (tile + 1)]
    return total


def kernel(
    geno_hbm, rhs_hbm, centre_hbm, spread_hbm, solution_ref, stats_ref,
    geno, r_0, r_1, r_2, packed, u_0, u_1, from_y_0, from_y_1, to_z_0, to_z_1,
    from_z_0, from_z_1, partial, acc, loads_out, from_core, by_x, loads_in,
    scalars, lhs, dir_loads, steps, betas,
    from_side, turned, rhs_ref, centre_ref, spread_ref, small_sem, geno_sem, s_gz, s_gy, s_gn, s_ry, s_rn, s_rz, s_core, s_x, s_back, s_sc,
    gz, gy, ry, rn, rz, core_sem, x_sem, back_sem, sc_sem,
):
    samp, snp = lax.axis_index("samp"), lax.axis_index("snp")
    x, core = samp // 2, samp % 2
    y, z = snp // NZ, snp % NZ
    residuals = (r_0, r_1, r_2)

    def at_z(other):
        return (samp, y * NZ + other)

    def at_y(other):
        return (samp, other * NZ + z)

    def at_x(other):
        return (other * 2 + core, snp)

    partner = (x * 2 + 1 - core, snp)

    def send(source, target, send_sem, recv_sem, device):
        pltpu.make_async_remote_copy(
            source, target, send_sem, recv_sem, device_id=device, device_id_type=MESH
        ).start()

    def settle(sem, like):
        pltpu.make_async_copy(like, like, sem).wait()

    piece = r_0.at[0:8, 0:CHUNK]
    pieces = r_0.at[0:24, 0:CHUNK]

    def rows_of(group):
        return pl.ds(pl.multiple_of(group * 8, 8), 8)

    def cols_of(chunk):
        return pl.ds(pl.multiple_of(chunk * CHUNK, 128), CHUNK)

    barrier = pltpu.get_barrier_semaphore()

    def greet(offset, carry):
        pl.semaphore_signal(
            barrier, inc=1, device_id=(samp, (snp + offset) % PEERS), device_id_type=MESH
        )
        return carry

    lax.fori_loop(1, PEERS, greet, 0)
    pl.semaphore_signal(barrier, inc=1, device_id=partner, device_id_type=MESH)
    for dx in range(1, NX):
        pl.semaphore_signal(barrier, inc=1, device_id=at_x((x + dx) % NX), device_id_type=MESH)

    small = (
        (rhs_hbm, rhs_ref), (centre_hbm, centre_ref.at[0]), (spread_hbm, spread_ref.at[0])
    )
    for which, (source, target) in enumerate(small):
        pltpu.make_async_copy(source, target, small_sem.at[which]).start()

    def main_cols(yy, zz):
        return pl.ds(pl.multiple_of(zz * CHUNK + yy * 128, 128), 128)

    for which, (source, target) in enumerate(small):
        pltpu.make_async_copy(source, target, small_sem.at[which]).wait()
    r_0[:, main_cols(y, z)] = rhs_ref[:, 0:128]
    tails = [rhs_ref[8 * group : 8 * group + 8, 128:160] for group in range(4)]
    packed[y, z] = jnp.concatenate(tails, axis=1)
    for zz in range(NZ):
        for yy in range(NY):
            first = 160 * (yy * NZ + zz)
            pltpu.make_async_copy(
                geno_hbm.at[pl.ds(first, 128)], geno.at[pl.ds(CHUNK * zz + 128 * yy, 128)], geno_sem
            ).start()
            pltpu.make_async_copy(
                geno_hbm.at[pl.ds(first + 128, 32)],
                geno.at[pl.ds(CHUNK * zz + 512 + 32 * yy, 32)],
                geno_sem,
            ).start()

    pl.semaphore_wait(barrier, PEERS - 1 + NX)

    def send_piece(k, yy, zz, send_sem, recv_sem, device):
        if k == 0:
            block = r_0.at[:, main_cols(yy, zz)]
            send(block, block, send_sem, recv_sem, device)
            send(packed.at[yy, zz], packed.at[yy, zz], send_sem, recv_sem, device)
        else:
            block = residuals[k].at[rows_of(yy), cols_of(zz)]
            send(block, block, send_sem, recv_sem, device)

    def forward(k, zz):
        for dy in (2, 1, 3):
            send_piece(k, y, zz, s_gy.at[k], gy.at[k, zz], at_y((y + dy) % NY))

    def pass_forward(k, d):
        settle(gz.at[k, d - 1], piece)
        forward(k, (z - d + NZ) % NZ)

    def gather(k):
        forward(k, z)
        for d in FAR + (1, 7):
            send_piece(k, y, z, s_gz.at[k], gz.at[k, d - 1], at_z((z + d) % NZ))
        settle(gy.at[k, z], pieces)
        for dy in range(1, NY):
            for d in (1, 7):
                other = at_z((z + d) % NZ)
                send_piece(k, (y + dy) % NY, z, s_gn.at[k], gy.at[k, z], other)
        partial[...] = jnp.zeros_like(partial)
        acc[...] = jnp.zeros_like(acc)
        for d in FAR[:2]:
            pass_forward(k, d)

    lane = lax.broadcasted_iota(jnp.int32, (8, 128), 1)

    def unpack(zz):
        sources = [packed[yy, zz] for yy in range(NY)]
        for group in range(4):
            tile = jnp.zeros((8, 128), f32)
            for yy in range(NY):
                shift = (32 * (yy - group)) % 128
                moved = pltpu.roll(sources[yy], shift, 1) if shift else sources[yy]
                tile = jnp.where(lane // 32 == yy, moved, tile)
            start = pl.multiple_of(zz * CHUNK + 512, 128)
            r_0[8 * group : 8 * group + 8, pl.ds(start, 128)] = tile

    def multiply_in(k, zz):
        if k == 0:
            unpack(zz)
        value = residuals[k][:, cols_of(zz)]
        high, low = split(value)
        partial[...] += jnp.dot(
            jnp.concatenate([high, low], axis=0), geno[cols_of(zz), :], preferred_element_type=f32
        )
        acc[0] += lanes_summed(high.astype(f32) + low.astype(f32))
        acc[1] += lanes_summed(value * value)
        if k > 0:
            acc[2] += lanes_summed(value * residuals[k - 1][:, cols_of(zz)])
        if k > 1:
            acc[3] += lanes_summed(value * r_0[:, cols_of(zz)])

    def to_loads(k):
        def chunk(step, carry):
            zz = (z - near(step) + NZ) % NZ

            @pl.when(step > 0)
            def _():
                settle(gy.at[k, zz], pieces)

            multiply_in(k, zz)

            @pl.when(step == 0)
            def _():
                for d in FAR[2:]:
                    pass_forward(k, d)
                for d in (1, 7):
                    settle(gz.at[k, d - 1], piece)

            return carry

        lax.fori_loop(0, NZ, chunk, 0)

    lane32 = lax.broadcasted_iota(jnp.int32, (ROWS, 128), 1)
    eye = lax.broadcasted_iota(jnp.int32, (ROWS, 128), 0) == lane32

    def turn(zz, carry):
        for first in range(0, COLS, 256):
            turned[first : first + 256, cols_of(zz)] = geno[cols_of(zz), first : first + 256].T
        return carry

    def over_samp(k):
        out, got, halves, full = loads_out.at[k], from_core.at[k], by_x.at[k], loads_in.at[k]
        total = jnp.sum(acc[0], axis=1, keepdims=True)
        raw = partial[0:ROWS] + partial[ROWS : 2 * ROWS]
        out[:, 0:COLS] = (raw - total * centre_ref[...]) / spread_ref[...]
        tile = jnp.zeros((ROWS, 128), f32)
        for which in range(1, 2 + k):
            tile = jnp.where(lane32 == which - 1, jnp.sum(acc[which], axis=1, keepdims=True), tile)
        out[:, COLS:WIDE] = tile
        mine = pl.ds(pl.multiple_of(core * 16, 16), 16)
        theirs = pl.ds(pl.multiple_of(16 - core * 16, 16), 16)
        send(out.at[theirs], got, s_core.at[k], core_sem.at[k], partner)
        settle(core_sem.at[k], got)
        halves[x] = out[mine, :] + got[...]
        for dx in (2, 1, 3):
            send(halves.at[x], halves.at[x], s_x.at[k], x_sem.at[k], at_x((x + dx) % NX))
        if k == 0:
            lax.fori_loop(0, NZ, turn, 0)
        settle(x_sem.at[k], halves.at[0:3])
        full[mine, :] = (halves[0] + halves[1]) + (halves[2] + halves[3])
        send(full.at[mine], full.at[mine], s_back.at[k], back_sem.at[k], partner)
        settle(back_sem.at[k], full.at[mine])

    def spread_norms(k):
        loads = dir_loads[...]
        norm = jnp.sum(lanes_summed(loads * loads), axis=1, keepdims=True)
        row = jnp.sum(jnp.where(eye, norm, 0.0), axis=0, keepdims=True)
        scalars[k, snp] = row

        slot = scalars.at[k, snp]
        for dz in (4, 3, 5, 2, 6, 1, 7, 0):
            for dy in (2, 1, 3, 0):
                if dy or dz:
                    other = (samp, (y + dy) % NY * NZ + (z + dz) % NZ)
                    send(slot, slot, s_sc.at[k], sc_sem.at[k], other)

    def total_norms(k):
        settle(sc_sem.at[k], scalars.at[k, 0 : PEERS - 1])
        row = jnp.sum(scalars[k], axis=0)
        return jnp.sum(jnp.where(eye, row, 0.0), axis=1, keepdims=True)

    def to_image(k):
        image, from_y, to_z, from_z = (
            (u_0, from_y_0, to_z_0, from_z_0), (u_1, from_y_1, to_z_1, from_z_1)
        )[k]
        high, low = split(dir_loads[...] / spread_ref[...])
        lhs[0:ROWS] = high
        lhs[ROWS : 2 * ROWS] = low
        shift = (high.astype(f32) + low.astype(f32)) * centre_ref[...]
        shift = jnp.sum(lanes_summed(shift), axis=1, keepdims=True)

        def multiply(offset):
            zz = (z + offset) % NZ
            both = jnp.dot(lhs[...], turned[:, cols_of(zz)], preferred_element_type=f32)
            image[:, cols_of(zz)] = both[0:ROWS] + both[ROWS : 2 * ROWS] - shift

        def along_y(zz):
            for dy in (2, 1, 3):
                other = (y + dy) % NY
                send(
                    image.at[rows_of(other), cols_of(zz)], from_y.at[dy - 1, :, cols_of(zz)],
                    s_ry.at[k], ry.at[k, zz], at_y(other),
                )

        def chunk(step, carry):
            offset = scatter_order(step)
            multiply(offset)
            zz = (z + offset) % NZ
            beside = (offset == 1) | (offset == 7)

            @pl.when(beside)
            def _():
                send(
                    image.at[:, cols_of(zz)], from_side.at[k, offset // 4],
                    s_rn.at[k], rn.at[k], at_z(zz),
                )

            @pl.when((offset != 0) & ~beside)
            def _():
                along_y(zz)

            return carry

        lax.fori_loop(0, NZ, chunk, 0)
        spread_norms(k)

        def of_y(zz):
            settle(ry.at[k, zz], pieces)
            total = image[rows_of(y), cols_of(zz)]
            for dy in range(NY - 1):
                total = total + from_y[dy, :, cols_of(zz)]
            return total

        def pass_on(offset):
            zz = (z + offset) % NZ
            to_z[zz] = of_y(zz)
            send(to_z.at[zz], from_z.at[offset - 2], s_rz.at[k], rz.at[k], at_z(zz))

        for offset in (4, 3, 5):
            pass_on(offset)
        settle(rn.at[k], from_side.at[k])
        image[:, cols_of(z)] += from_side[k, 0] + from_side[k, 1]
        along_y(z)
        for offset in (2, 6):
            pass_on(offset)
        total = of_y(z)
        settle(rz.at[k], from_z)
        for slot in range(NZ - 3):
            total = total + from_z[slot]
        return total

    norms, squares = [], []
    for k in range(ROUNDS):
        gather(k)
        if k == 0:
            settle(geno_sem, geno)
        to_loads(k)
        over_samp(k)
        loads = loads_in[k, :, 0:COLS]
        norm = loads_in[k, :, COLS : COLS + 1]
        if k == 0:
            dir_loads[...] = loads
            square = norm
        else:
            beta = norm / norms[-1]
            dir_loads[...] = loads + beta * dir_loads[...]
            cross = loads_in[k, :, COLS + 1 : COLS + 2]
            if k == 2:
                cross = cross + betas[0][:, 0:1] * loads_in[k, :, COLS + 2 : COLS + 3]
            square = norm + 2.0 * beta * cross + beta * beta * squares[-1]
            betas[k - 1] = jnp.broadcast_to(beta, (ROWS, 128))
        norms.append(norm)
        squares.append(square)
        if k < ROUNDS - 1:
            summed = to_image(k)
        else:
            spread_norms(k)
        size = norm / (total_norms(k) * (1.0 / MARKERS) + RIDGE * square)
        steps[k] = jnp.broadcast_to(size, (ROWS, 128))
        gain = size * (1.0 / math.sqrt(SAMPLES))
        if k == 0:
            stats_ref[...] = gain * dir_loads[...]
        else:
            stats_ref[...] += gain * dir_loads[...]
        if k < ROUNDS - 1:
            mine = (rows_of(y), cols_of(z))
            direction = residuals[k][mine]
            if k == 1:
                direction = direction + betas[0, rows_of(y), 0:1] * r_0[mine]
            moved = summed * (1.0 / MARKERS) + RIDGE * direction
            residuals[k + 1][mine] = residuals[k][mine] - steps[k, rows_of(y), 0:1] * moved

    def combined(columns):
        first = r_0[:, columns]
        second = r_1[:, columns] + betas[0][:, 0:1] * first
        third = r_2[:, columns] + betas[1][:, 0:1] * second
        return steps[0][:, 0:1] * first + steps[1][:, 0:1] * second + steps[2][:, 0:1] * third

    solution_ref[:, 0:128] = combined(main_cols(y, z))
    tail = combined(pl.ds(pl.multiple_of(z * CHUNK + 512, 128), 128))
    for yy in range(NY):

        @pl.when(y == yy)
        def _():
            solution_ref[:, 128:160] = tail[:, 32 * yy : 32 * yy + 32]

    for k in range(ROUNDS):
        settle(s_gz.at[k], r_0.at[0:8, 0 : 7 * CHUNK])
        settle(s_gy.at[k], r_0.at[0:24, 0 : 6 * CHUNK])
        settle(s_gn.at[k], r_0.at[0:24, 0 : 2 * CHUNK])
        settle(s_core.at[k], from_core.at[k])
        settle(s_x.at[k], by_x.at[k, 0:3])
        settle(s_back.at[k], from_core.at[k])
        settle(s_sc.at[k], scalars.at[k, 0 : PEERS - 1])
    for k in range(ROUNDS - 1):
        settle(s_ry.at[k], r_0.at[0:24, 0 : 6 * CHUNK])
        settle(s_rn.at[k], from_side.at[k])
        settle(s_rz.at[k], from_z_0)


def local(genotype, centre, spread, pheno_probes):
    block = (ROWS, BLOCK)
    dma = pltpu.SemaphoreType.DMA
    vmem = pl.BlockSpec(memory_space=pltpu.VMEM)
    return pl.pallas_call(
        kernel,
        out_shape=(
            jax.ShapeDtypeStruct((ROWS, 160), f32),
            jax.ShapeDtypeStruct((ROWS, COLS), f32),
        ),
        in_specs=[pl.BlockSpec(memory_space=pl.ANY)] * 4,
        out_specs=(vmem, vmem),
        scratch_shapes=[
            pltpu.VMEM((BLOCK, COLS), jnp.bfloat16),
            pltpu.VMEM(block, f32),
            pltpu.VMEM(block, f32),
            pltpu.VMEM(block, f32),
            pltpu.VMEM((NY, NZ, 8, 128), f32),
            pltpu.VMEM(block, f32),
            pltpu.VMEM(block, f32),
            pltpu.VMEM((NY - 1, 8, BLOCK), f32),
            pltpu.VMEM((NY - 1, 8, BLOCK), f32),
            pltpu.VMEM((NZ, 8, CHUNK), f32),
            pltpu.VMEM((NZ, 8, CHUNK), f32),
            pltpu.VMEM((NZ - 3, 8, CHUNK), f32),
            pltpu.VMEM((NZ - 3, 8, CHUNK), f32),
            pltpu.VMEM((2 * ROWS, COLS), f32),
            pltpu.VMEM((4, ROWS, 128), f32),
            pltpu.VMEM((ROUNDS, ROWS, WIDE), f32),
            pltpu.VMEM((ROUNDS, 16, WIDE), f32),
            pltpu.VMEM((ROUNDS, NX, 16, WIDE), f32),
            pltpu.VMEM((ROUNDS, ROWS, WIDE), f32),
            pltpu.VMEM((ROUNDS, PEERS, 1, 128), f32),
            pltpu.VMEM((2 * ROWS, COLS), jnp.bfloat16),
            pltpu.VMEM((ROWS, COLS), f32),
            pltpu.VMEM((ROUNDS, ROWS, 128), f32),
            pltpu.VMEM((ROUNDS - 1, ROWS, 128), f32),
            pltpu.VMEM((ROUNDS - 1, 2, ROWS, CHUNK), f32),
            pltpu.VMEM((COLS, BLOCK), jnp.bfloat16),
            pltpu.VMEM((ROWS, 160), f32),
            pltpu.VMEM((1, COLS), f32),
            pltpu.VMEM((1, COLS), f32),
            dma((3,)),
            dma,
            dma((ROUNDS,)),
            dma((ROUNDS,)),
            dma((ROUNDS,)),
            dma((ROUNDS - 1,)),
            dma((ROUNDS - 1,)),
            dma((ROUNDS - 1,)),
            dma((ROUNDS,)),
            dma((ROUNDS,)),
            dma((ROUNDS,)),
            dma((ROUNDS,)),
            dma((ROUNDS, NZ - 1)),
            dma((ROUNDS, NZ)),
            dma((ROUNDS - 1, NZ)),
            dma((ROUNDS - 1,)),
            dma((ROUNDS - 1,)),
            dma((ROUNDS,)),
            dma((ROUNDS,)),
            dma((ROUNDS,)),
            dma((ROUNDS,)),
        ],
        compiler_params=pltpu.CompilerParams(
            collective_id=0, has_side_effects=True, vmem_limit_bytes=60 * 1024 * 1024
        ),
        name="conjugate_gradients",
    )(genotype, pheno_probes, centre, spread)


def solution(mesh):
    in_specs = (P("samp", "snp"), P("snp"), P("snp"), P(None, ("samp", "snp")))
    out_specs = (P(None, ("samp", "snp")), P(None, "snp"))
    return jax.shard_map(local, mesh=mesh, in_specs=in_specs, out_specs=out_specs, check_vma=False)
```

```python
import math

import jax
import jax.numpy as jnp
from jax import lax
from jax.experimental import pallas as pl
from jax.experimental.pallas import tpu as pltpu
from jax.sharding import PartitionSpec as P

SAMPLES = 40960
MARKERS = 40960
ROUNDS = 3
RIDGE = 0.1

ROWS = 32
NY, NZ = 4, 8
NX = 4
PEERS = NY * NZ
CHUNK = 640
BLOCK = CHUNK * NZ
COLS = 1280
WIDE = COLS + 128
PIECE = 8 * CHUNK

MESH = pl.DeviceIdType.MESH
FAR = (2, 6, 3, 5, 4)
SCATTER = (4, 3, 5, 1, 7, 2, 6, 0)
f32 = jnp.float32


def near(step):
    half = (step + 1) // 2
    return jnp.where(step % 2 == 1, half, (NZ - half) % NZ)


def scatter_order(step):
    offset = jnp.int32(SCATTER[0])
    for place in range(1, NZ):
        offset = jnp.where(step == place, SCATTER[place], offset)
    return offset


def split(value):
    high = value.astype(jnp.bfloat16)
    rest = value - high.astype(f32)
    return high, rest.astype(jnp.bfloat16)


def lanes_summed(value):
    total = value[:, 0:128]
    for tile in range(1, value.shape[1] // 128):
        total = total + value[:, 128 * tile : 128 * (tile + 1)]
    return total


def kernel(
    geno_hbm, rhs_hbm, centre_hbm, spread_hbm, solution_ref, stats_ref,
    geno, r_0, r_1, r_2, packed, u_0, u_1, from_y_0, from_y_1, to_z_0, to_z_1,
    from_z_0, from_z_1, partial, acc, loads_out, from_core, by_x, loads_in,
    scalars, lhs, dir_loads, steps, betas,
    from_side, turned, rhs_ref, centre_ref, spread_ref, small_sem, geno_sem, s_gz, s_gy, s_gn, s_ry, s_rn, s_rz, s_core, s_x, s_back, s_sc,
    gz, gy, ry, rn, rz, core_sem, x_sem, back_sem, sc_sem,
):
    samp, snp = lax.axis_index("samp"), lax.axis_index("snp")
    x, core = samp // 2, samp % 2
    y, z = snp // NZ, snp % NZ
    residuals = (r_0, r_1, r_2)

    def at_z(other):
        return (samp, y * NZ + other)

    def at_y(other):
        return (samp, other * NZ + z)

    def at_x(other):
        return (other * 2 + core, snp)

    partner = (x * 2 + 1 - core, snp)

    def send(source, target, send_sem, recv_sem, device):
        pltpu.make_async_remote_copy(
            source, target, send_sem, recv_sem, device_id=device, device_id_type=MESH
        ).start()

    def settle(sem, like):
        pltpu.make_async_copy(like, like, sem).wait()

    piece = r_0.at[0:8, 0:CHUNK]
    pieces = r_0.at[0:24, 0:CHUNK]

    def rows_of(group):
        return pl.ds(pl.multiple_of(group * 8, 8), 8)

    def cols_of(chunk):
        return pl.ds(pl.multiple_of(chunk * CHUNK, 128), CHUNK)

    barrier = pltpu.get_barrier_semaphore()

    greeted = [at_z((z + d) % NZ) for d in (4, 3, 5, 2, 6)]
    greeted += [at_y((y + dy) % NY) for dy in (2, 1, 3)]
    greeted += [at_x((x + dx) % NX) for dx in (2, 1, 3)]
    greeted += [at_z((z + d) % NZ) for d in (1, 7)] + [partner]
    for other in greeted:
        pl.semaphore_signal(barrier, inc=1, device_id=other, device_id_type=MESH)
    small = (
        (rhs_hbm, rhs_ref), (centre_hbm, centre_ref.at[0]), (spread_hbm, spread_ref.at[0])
    )
    for which, (source, target) in enumerate(small):
        pltpu.make_async_copy(source, target, small_sem.at[which]).start()

    def main_cols(yy, zz):
        return pl.ds(pl.multiple_of(zz * CHUNK + yy * 128, 128), 128)

    for which, (source, target) in enumerate(small):
        pltpu.make_async_copy(source, target, small_sem.at[which]).wait()
    r_0[:, main_cols(y, z)] = rhs_ref[:, 0:128]
    tails = [rhs_ref[8 * group : 8 * group + 8, 128:160] for group in range(4)]
    packed[y, z] = jnp.concatenate(tails, axis=1)
    for zz in range(NZ):
        for yy in range(NY):
            first = 160 * (yy * NZ + zz)
            pltpu.make_async_copy(
                geno_hbm.at[pl.ds(first, 128)], geno.at[pl.ds(CHUNK * zz + 128 * yy, 128)], geno_sem
            ).start()
            pltpu.make_async_copy(
                geno_hbm.at[pl.ds(first + 128, 32)],
                geno.at[pl.ds(CHUNK * zz + 512 + 32 * yy, 32)],
                geno_sem,
            ).start()

    pl.semaphore_wait(barrier, len(greeted))

    def send_piece(k, yy, zz, send_sem, recv_sem, device):
        if k == 0:
            block = r_0.at[:, main_cols(yy, zz)]
            send(block, block, send_sem, recv_sem, device)
            send(packed.at[yy, zz], packed.at[yy, zz], send_sem, recv_sem, device)
        else:
            block = residuals[k].at[rows_of(yy), cols_of(zz)]
            send(block, block, send_sem, recv_sem, device)

    def forward(k, zz):
        for dy in (2, 1, 3):
            send_piece(k, y, zz, s_gy.at[k], gy.at[k, zz], at_y((y + dy) % NY))

    def pass_forward(k, d):
        settle(gz.at[k, d - 1], piece)
        forward(k, (z - d + NZ) % NZ)

    def gather(k):
        forward(k, z)
        for d in FAR + (1, 7):
            send_piece(k, y, z, s_gz.at[k], gz.at[k, d - 1], at_z((z + d) % NZ))
        settle(gy.at[k, z], pieces)
        for dy in range(1, NY):
            for d in (1, 7):
                other = at_z((z + d) % NZ)
                send_piece(k, (y + dy) % NY, z, s_gn.at[k], gy.at[k, z], other)
        partial[...] = jnp.zeros_like(partial)
        acc[...] = jnp.zeros_like(acc)
        for d in FAR[:2]:
            pass_forward(k, d)

    lane = lax.broadcasted_iota(jnp.int32, (8, 128), 1)

    def unpack(zz):
        sources = [packed[yy, zz] for yy in range(NY)]
        for group in range(4):
            tile = jnp.zeros((8, 128), f32)
            for yy in range(NY):
                shift = (32 * (yy - group)) % 128
                moved = pltpu.roll(sources[yy], shift, 1) if shift else sources[yy]
                tile = jnp.where(lane // 32 == yy, moved, tile)
            start = pl.multiple_of(zz * CHUNK + 512, 128)
            r_0[8 * group : 8 * group + 8, pl.ds(start, 128)] = tile

    def multiply_in(k, zz):
        if k == 0:
            unpack(zz)
        value = residuals[k][:, cols_of(zz)]
        high, low = split(value)
        partial[...] += jnp.dot(
            jnp.concatenate([high, low], axis=0), geno[cols_of(zz), :], preferred_element_type=f32
        )
        acc[0] += lanes_summed(high.astype(f32) + low.astype(f32))
        acc[1] += lanes_summed(value * value)
        if k > 0:
            acc[2] += lanes_summed(value * residuals[k - 1][:, cols_of(zz)])
        if k > 1:
            acc[3] += lanes_summed(value * r_0[:, cols_of(zz)])

    def to_loads(k):
        def chunk(step, carry):
            zz = (z - near(step) + NZ) % NZ

            @pl.when(step > 0)
            def _():
                settle(gy.at[k, zz], pieces)

            multiply_in(k, zz)

            @pl.when(step == 0)
            def _():
                for d in FAR[2:]:
                    pass_forward(k, d)
                for d in (1, 7):
                    settle(gz.at[k, d - 1], piece)

            return carry

        lax.fori_loop(0, NZ, chunk, 0)

    lane32 = lax.broadcasted_iota(jnp.int32, (ROWS, 128), 1)
    eye = lax.broadcasted_iota(jnp.int32, (ROWS, 128), 0) == lane32

    def turn(zz, carry):
        for first in range(0, COLS, 256):
            turned[first : first + 256, cols_of(zz)] = geno[cols_of(zz), first : first + 256].T
        return carry

    def over_samp(k):
        out, got, halves, full = loads_out.at[k], from_core.at[k], by_x.at[k], loads_in.at[k]
        total = jnp.sum(acc[0], axis=1, keepdims=True)
        raw = partial[0:ROWS] + partial[ROWS : 2 * ROWS]
        out[:, 0:COLS] = (raw - total * centre_ref[...]) / spread_ref[...]
        tile = jnp.zeros((ROWS, 128), f32)
        for which in range(1, 2 + k):
            tile = jnp.where(lane32 == which - 1, jnp.sum(acc[which], axis=1, keepdims=True), tile)
        out[:, COLS:WIDE] = tile
        mine = pl.ds(pl.multiple_of(core * 16, 16), 16)
        theirs = pl.ds(pl.multiple_of(16 - core * 16, 16), 16)
        send(out.at[theirs], got, s_core.at[k], core_sem.at[k], partner)
        settle(core_sem.at[k], got)
        halves[x] = out[mine, :] + got[...]
        for dx in (2, 1, 3):
            send(halves.at[x], halves.at[x], s_x.at[k], x_sem.at[k], at_x((x + dx) % NX))
        if k == 0:
            lax.fori_loop(0, NZ, turn, 0)
        settle(x_sem.at[k], halves.at[0:3])
        full[mine, :] = (halves[0] + halves[1]) + (halves[2] + halves[3])
        send(full.at[mine], full.at[mine], s_back.at[k], back_sem.at[k], partner)
        settle(back_sem.at[k], full.at[mine])

    def spread_norms(k):
        loads = dir_loads[...]
        norm = jnp.sum(lanes_summed(loads * loads), axis=1, keepdims=True)
        row = jnp.sum(jnp.where(eye, norm, 0.0), axis=0, keepdims=True)
        scalars[k, snp] = row

        slot = scalars.at[k, snp]
        for dz in (4, 3, 5, 2, 6, 1, 7, 0):
            for dy in (2, 1, 3, 0):
                if dy or dz:
                    other = (samp, (y + dy) % NY * NZ + (z + dz) % NZ)
                    send(slot, slot, s_sc.at[k], sc_sem.at[k], other)

    def total_norms(k):
        settle(sc_sem.at[k], scalars.at[k, 0 : PEERS - 1])
        row = jnp.sum(scalars[k], axis=0)
        return jnp.sum(jnp.where(eye, row, 0.0), axis=1, keepdims=True)

    def to_image(k):
        image, from_y, to_z, from_z = (
            (u_0, from_y_0, to_z_0, from_z_0), (u_1, from_y_1, to_z_1, from_z_1)
        )[k]
        high, low = split(dir_loads[...] / spread_ref[...])
        lhs[0:ROWS] = high
        lhs[ROWS : 2 * ROWS] = low
        shift = (high.astype(f32) + low.astype(f32)) * centre_ref[...]
        shift = jnp.sum(lanes_summed(shift), axis=1, keepdims=True)

        def multiply(offset):
            zz = (z + offset) % NZ
            both = jnp.dot(lhs[...], turned[:, cols_of(zz)], preferred_element_type=f32)
            image[:, cols_of(zz)] = both[0:ROWS] + both[ROWS : 2 * ROWS] - shift

        def along_y(zz):
            for dy in (2, 1, 3):
                other = (y + dy) % NY
                send(
                    image.at[rows_of(other), cols_of(zz)], from_y.at[dy - 1, :, cols_of(zz)],
                    s_ry.at[k], ry.at[k, zz], at_y(other),
                )

        def chunk(step, carry):
            offset = scatter_order(step)
            multiply(offset)
            zz = (z + offset) % NZ
            beside = (offset == 1) | (offset == 7)

            @pl.when(beside)
            def _():
                send(
                    image.at[:, cols_of(zz)], from_side.at[k, offset // 4],
                    s_rn.at[k], rn.at[k], at_z(zz),
                )

            @pl.when((offset != 0) & ~beside)
            def _():
                along_y(zz)

            return carry

        lax.fori_loop(0, NZ, chunk, 0)
        spread_norms(k)

        def of_y(zz):
            settle(ry.at[k, zz], pieces)
            total = image[rows_of(y), cols_of(zz)]
            for dy in range(NY - 1):
                total = total + from_y[dy, :, cols_of(zz)]
            return total

        def pass_on(offset):
            zz = (z + offset) % NZ
            to_z[zz] = of_y(zz)
            send(to_z.at[zz], from_z.at[offset - 2], s_rz.at[k], rz.at[k], at_z(zz))

        for offset in (4, 3, 5):
            pass_on(offset)
        settle(rn.at[k], from_side.at[k])
        image[:, cols_of(z)] += from_side[k, 0] + from_side[k, 1]
        along_y(z)
        for offset in (2, 6):
            pass_on(offset)
        total = of_y(z)
        settle(rz.at[k], from_z)
        for slot in range(NZ - 3):
            total = total + from_z[slot]
        return total

    norms, squares = [], []
    for k in range(ROUNDS):
        gather(k)
        if k == 0:
            settle(geno_sem, geno)
        to_loads(k)
        over_samp(k)
        loads = loads_in[k, :, 0:COLS]
        norm = loads_in[k, :, COLS : COLS + 1]
        if k == 0:
            dir_loads[...] = loads
            square = norm
        else:
            beta = norm / norms[-1]
            dir_loads[...] = loads + beta * dir_loads[...]
            cross = loads_in[k, :, COLS + 1 : COLS + 2]
            if k == 2:
                cross = cross + betas[0][:, 0:1] * loads_in[k, :, COLS + 2 : COLS + 3]
            square = norm + 2.0 * beta * cross + beta * beta * squares[-1]
            betas[k - 1] = jnp.broadcast_to(beta, (ROWS, 128))
        norms.append(norm)
        squares.append(square)
        if k < ROUNDS - 1:
            summed = to_image(k)
        else:
            spread_norms(k)
        size = norm / (total_norms(k) * (1.0 / MARKERS) + RIDGE * square)
        steps[k] = jnp.broadcast_to(size, (ROWS, 128))
        gain = size * (1.0 / math.sqrt(SAMPLES))
        if k == 0:
            stats_ref[...] = gain * dir_loads[...]
        else:
            stats_ref[...] += gain * dir_loads[...]
        if k < ROUNDS - 1:
            mine = (rows_of(y), cols_of(z))
            direction = residuals[k][mine]
            if k == 1:
                direction = direction + betas[0, rows_of(y), 0:1] * r_0[mine]
            moved = summed * (1.0 / MARKERS) + RIDGE * direction
            residuals[k + 1][mine] = residuals[k][mine] - steps[k, rows_of(y), 0:1] * moved

    def combined(columns):
        first = r_0[:, columns]
        second = r_1[:, columns] + betas[0][:, 0:1] * first
        third = r_2[:, columns] + betas[1][:, 0:1] * second
        return steps[0][:, 0:1] * first + steps[1][:, 0:1] * second + steps[2][:, 0:1] * third

    solution_ref[:, 0:128] = combined(main_cols(y, z))
    tail = combined(pl.ds(pl.multiple_of(z * CHUNK + 512, 128), 128))
    for yy in range(NY):

        @pl.when(y == yy)
        def _():
            solution_ref[:, 128:160] = tail[:, 32 * yy : 32 * yy + 32]

    for k in range(ROUNDS):
        settle(s_gz.at[k], r_0.at[0:8, 0 : 7 * CHUNK])
        settle(s_gy.at[k], r_0.at[0:24, 0 : 6 * CHUNK])
        settle(s_gn.at[k], r_0.at[0:24, 0 : 2 * CHUNK])
        settle(s_core.at[k], from_core.at[k])
        settle(s_x.at[k], by_x.at[k, 0:3])
        settle(s_back.at[k], from_core.at[k])
        settle(s_sc.at[k], scalars.at[k, 0 : PEERS - 1])
    for k in range(ROUNDS - 1):
        settle(s_ry.at[k], r_0.at[0:24, 0 : 6 * CHUNK])
        settle(s_rn.at[k], from_side.at[k])
        settle(s_rz.at[k], from_z_0)


def local(genotype, centre, spread, pheno_probes):
    block = (ROWS, BLOCK)
    dma = pltpu.SemaphoreType.DMA
    vmem = pl.BlockSpec(memory_space=pltpu.VMEM)
    return pl.pallas_call(
        kernel,
        out_shape=(
            jax.ShapeDtypeStruct((ROWS, 160), f32),
            jax.ShapeDtypeStruct((ROWS, COLS), f32),
        ),
        in_specs=[pl.BlockSpec(memory_space=pl.ANY)] * 4,
        out_specs=(vmem, vmem),
        scratch_shapes=[
            pltpu.VMEM((BLOCK, COLS), jnp.bfloat16),
            pltpu.VMEM(block, f32),
            pltpu.VMEM(block, f32),
            pltpu.VMEM(block, f32),
            pltpu.VMEM((NY, NZ, 8, 128), f32),
            pltpu.VMEM(block, f32),
            pltpu.VMEM(block, f32),
            pltpu.VMEM((NY - 1, 8, BLOCK), f32),
            pltpu.VMEM((NY - 1, 8, BLOCK), f32),
            pltpu.VMEM((NZ, 8, CHUNK), f32),
            pltpu.VMEM((NZ, 8, CHUNK), f32),
            pltpu.VMEM((NZ - 3, 8, CHUNK), f32),
            pltpu.VMEM((NZ - 3, 8, CHUNK), f32),
            pltpu.VMEM((2 * ROWS, COLS), f32),
            pltpu.VMEM((4, ROWS, 128), f32),
            pltpu.VMEM((ROUNDS, ROWS, WIDE), f32),
            pltpu.VMEM((ROUNDS, 16, WIDE), f32),
            pltpu.VMEM((ROUNDS, NX, 16, WIDE), f32),
            pltpu.VMEM((ROUNDS, ROWS, WIDE), f32),
            pltpu.VMEM((ROUNDS, PEERS, 1, 128), f32),
            pltpu.VMEM((2 * ROWS, COLS), jnp.bfloat16),
            pltpu.VMEM((ROWS, COLS), f32),
            pltpu.VMEM((ROUNDS, ROWS, 128), f32),
            pltpu.VMEM((ROUNDS - 1, ROWS, 128), f32),
            pltpu.VMEM((ROUNDS - 1, 2, ROWS, CHUNK), f32),
            pltpu.VMEM((COLS, BLOCK), jnp.bfloat16),
            pltpu.VMEM((ROWS, 160), f32),
            pltpu.VMEM((1, COLS), f32),
            pltpu.VMEM((1, COLS), f32),
            dma((3,)),
            dma,
            dma((ROUNDS,)),
            dma((ROUNDS,)),
            dma((ROUNDS,)),
            dma((ROUNDS - 1,)),
            dma((ROUNDS - 1,)),
            dma((ROUNDS - 1,)),
            dma((ROUNDS,)),
            dma((ROUNDS,)),
            dma((ROUNDS,)),
            dma((ROUNDS,)),
            dma((ROUNDS, NZ - 1)),
            dma((ROUNDS, NZ)),
            dma((ROUNDS - 1, NZ)),
            dma((ROUNDS - 1,)),
            dma((ROUNDS - 1,)),
            dma((ROUNDS,)),
            dma((ROUNDS,)),
            dma((ROUNDS,)),
            dma((ROUNDS,)),
        ],
        compiler_params=pltpu.CompilerParams(
            collective_id=0, has_side_effects=True, vmem_limit_bytes=60 * 1024 * 1024
        ),
        name="conjugate_gradients",
    )(genotype, pheno_probes, centre, spread)


def solution(mesh):
    in_specs = (P("samp", "snp"), P("snp"), P("snp"), P(None, ("samp", "snp")))
    out_specs = (P(None, ("samp", "snp")), P(None, "snp"))
    return jax.shard_map(local, mesh=mesh, in_specs=in_specs, out_specs=out_specs, check_vma=False)
```

```python
import math

import jax
import jax.numpy as jnp
from jax import lax
from jax.experimental import pallas as pl
from jax.experimental.pallas import tpu as pltpu
from jax.sharding import PartitionSpec as P

SAMPLES = 40960
MARKERS = 40960
ROUNDS = 3
RIDGE = 0.1

ROWS = 32
NY, NZ = 4, 8
NX = 4
PEERS = NY * NZ
CHUNK = 640
BLOCK = CHUNK * NZ
COLS = 1280
WIDE = COLS + 128
PIECE = 8 * CHUNK

MESH = pl.DeviceIdType.MESH
FAR = (2, 6, 3, 5, 4)
SCATTER = (4, 3, 5, 1, 7, 2, 6, 0)
f32 = jnp.float32


def near(step):
    half = (step + 1) // 2
    return jnp.where(step % 2 == 1, half, (NZ - half) % NZ)


def scatter_order(step):
    offset = jnp.int32(SCATTER[0])
    for place in range(1, NZ):
        offset = jnp.where(step == place, SCATTER[place], offset)
    return offset


def split(value):
    high = value.astype(jnp.bfloat16)
    rest = value - high.astype(f32)
    return high, rest.astype(jnp.bfloat16)


def lanes_summed(value):
    total = value[:, 0:128]
    for tile in range(1, value.shape[1] // 128):
        total = total + value[:, 128 * tile : 128 * (tile + 1)]
    return total


def kernel(
    geno_hbm, rhs_hbm, centre_hbm, spread_hbm, solution_ref, stats_ref,
    geno, r_0, r_1, r_2, packed, u_0, u_1, from_y_0, from_y_1, to_z_0, to_z_1,
    from_z_0, from_z_1, partial, acc, loads_out, from_core, by_x, loads_in,
    scalars, lhs, dir_loads, steps, betas,
    last, from_side, turned, rhs_ref, centre_ref, spread_ref, small_sem, geno_sem, s_gz, s_gy, s_gn, s_ry, s_rn, s_rz, s_core, s_x, s_back, s_sc,
    gz, gy, ry, rn, rz, core_sem, x_sem, back_sem, sc_sem,
):
    samp, snp = lax.axis_index("samp"), lax.axis_index("snp")
    x, core = samp // 2, samp % 2
    y, z = snp // NZ, snp % NZ
    residuals = (r_0, r_1, r_2)

    def at_z(other):
        return (samp, y * NZ + other)

    def at_y(other):
        return (samp, other * NZ + z)

    def at_x(other):
        return (other * 2 + core, snp)

    partner = (x * 2 + 1 - core, snp)

    def send(source, target, send_sem, recv_sem, device):
        pltpu.make_async_remote_copy(
            source, target, send_sem, recv_sem, device_id=device, device_id_type=MESH
        ).start()

    def settle(sem, like):
        pltpu.make_async_copy(like, like, sem).wait()

    piece = r_0.at[0:8, 0:CHUNK]
    pieces = r_0.at[0:24, 0:CHUNK]

    def rows_of(group):
        return pl.ds(pl.multiple_of(group * 8, 8), 8)

    def cols_of(chunk):
        return pl.ds(pl.multiple_of(chunk * CHUNK, 128), CHUNK)

    barrier = pltpu.get_barrier_semaphore()

    greeted = [at_z((z + d) % NZ) for d in (4, 3, 5, 2, 6)]
    greeted += [at_y((y + dy) % NY) for dy in (2, 1, 3)]
    greeted += [at_x((x + dx) % NX) for dx in (2, 1, 3)]
    greeted += [at_z((z + d) % NZ) for d in (1, 7)] + [partner]
    for other in greeted:
        pl.semaphore_signal(barrier, inc=1, device_id=other, device_id_type=MESH)
    small = (
        (rhs_hbm, rhs_ref), (centre_hbm, centre_ref.at[0]), (spread_hbm, spread_ref.at[0])
    )
    for which, (source, target) in enumerate(small):
        pltpu.make_async_copy(source, target, small_sem.at[which]).start()

    def main_cols(yy, zz):
        return pl.ds(pl.multiple_of(zz * CHUNK + yy * 128, 128), 128)

    for which, (source, target) in enumerate(small):
        pltpu.make_async_copy(source, target, small_sem.at[which]).wait()
    r_0[:, main_cols(y, z)] = rhs_ref[:, 0:128]
    tails = [rhs_ref[8 * group : 8 * group + 8, 128:160] for group in range(4)]
    packed[y, z] = jnp.concatenate(tails, axis=1)
    for zz in range(NZ):
        for yy in range(NY):
            first = 160 * (yy * NZ + zz)
            pltpu.make_async_copy(
                geno_hbm.at[pl.ds(first, 128)], geno.at[pl.ds(CHUNK * zz + 128 * yy, 128)], geno_sem
            ).start()
            pltpu.make_async_copy(
                geno_hbm.at[pl.ds(first + 128, 32)],
                geno.at[pl.ds(CHUNK * zz + 512 + 32 * yy, 32)],
                geno_sem,
            ).start()

    pl.semaphore_wait(barrier, len(greeted))

    def send_piece(k, yy, zz, send_sem, recv_sem, device):
        if k == 0:
            block = r_0.at[:, main_cols(yy, zz)]
            send(block, block, send_sem, recv_sem, device)
            send(packed.at[yy, zz], packed.at[yy, zz], send_sem, recv_sem, device)
        else:
            block = residuals[k].at[rows_of(yy), cols_of(zz)]
            send(block, block, send_sem, recv_sem, device)

    def forward(k, zz):
        for dy in (2, 1, 3):
            send_piece(k, y, zz, s_gy.at[k], gy.at[k, zz], at_y((y + dy) % NY))

    def pass_forward(k, d):
        settle(gz.at[k, d - 1], piece)
        forward(k, (z - d + NZ) % NZ)

    def gather(k):
        forward(k, z)
        for d in FAR + (1, 7):
            send_piece(k, y, z, s_gz.at[k], gz.at[k, d - 1], at_z((z + d) % NZ))
        settle(gy.at[k, z], pieces)
        for dy in range(1, NY):
            for d in (1, 7):
                other = at_z((z + d) % NZ)
                send_piece(k, (y + dy) % NY, z, s_gn.at[k], gy.at[k, z], other)
        partial[...] = jnp.zeros_like(partial)
        acc[...] = jnp.zeros_like(acc)
        for d in FAR[:2]:
            pass_forward(k, d)

    lane = lax.broadcasted_iota(jnp.int32, (8, 128), 1)

    def unpack(zz):
        sources = [packed[yy, zz] for yy in range(NY)]
        for group in range(4):
            tile = jnp.zeros((8, 128), f32)
            for yy in range(NY):
                shift = (32 * (yy - group)) % 128
                moved = pltpu.roll(sources[yy], shift, 1) if shift else sources[yy]
                tile = jnp.where(lane // 32 == yy, moved, tile)
            start = pl.multiple_of(zz * CHUNK + 512, 128)
            r_0[8 * group : 8 * group + 8, pl.ds(start, 128)] = tile

    def multiply_in(k, zz):
        if k == 0:
            unpack(zz)
        value = residuals[k][:, cols_of(zz)]
        high, low = split(value)
        partial[...] += jnp.dot(
            jnp.concatenate([high, low], axis=0), geno[cols_of(zz), :], preferred_element_type=f32
        )
        acc[0] += lanes_summed(high.astype(f32) + low.astype(f32))
        acc[1] += lanes_summed(value * value)
        if k > 0:
            acc[2] += lanes_summed(value * residuals[k - 1][:, cols_of(zz)])
        if k > 1:
            acc[3] += lanes_summed(value * r_0[:, cols_of(zz)])

    def to_loads(k):
        def chunk(step, carry):
            zz = (z - near(step) + NZ) % NZ

            @pl.when(step > 0)
            def _():
                settle(gy.at[k, zz], pieces)

            multiply_in(k, zz)

            @pl.when(step == 0)
            def _():
                for d in FAR[2:]:
                    pass_forward(k, d)
                for d in (1, 7):
                    settle(gz.at[k, d - 1], piece)

            return carry

        lax.fori_loop(0, NZ, chunk, 0)

    lane32 = lax.broadcasted_iota(jnp.int32, (ROWS, 128), 1)
    eye = lax.broadcasted_iota(jnp.int32, (ROWS, 128), 0) == lane32

    def turn(zz, carry):
        for first in range(0, COLS, 256):
            turned[first : first + 256, cols_of(zz)] = geno[cols_of(zz), first : first + 256].T
        return carry

    def over_samp(k):
        out, got, halves, full = loads_out.at[k], from_core.at[k], by_x.at[k], loads_in.at[k]
        total = jnp.sum(acc[0], axis=1, keepdims=True)
        raw = partial[0:ROWS] + partial[ROWS : 2 * ROWS]
        out[:, 0:COLS] = (raw - total * centre_ref[...]) / spread_ref[...]
        tile = jnp.zeros((ROWS, 128), f32)
        for which in range(1, 2 + k):
            tile = jnp.where(lane32 == which - 1, jnp.sum(acc[which], axis=1, keepdims=True), tile)
        out[:, COLS:WIDE] = tile
        mine = pl.ds(pl.multiple_of(core * 16, 16), 16)
        theirs = pl.ds(pl.multiple_of(16 - core * 16, 16), 16)
        send(out.at[theirs], got, s_core.at[k], core_sem.at[k], partner)
        settle(core_sem.at[k], got)
        halves[x] = out[mine, :] + got[...]
        for dx in (2, 1, 3):
            send(halves.at[x], halves.at[x], s_x.at[k], x_sem.at[k], at_x((x + dx) % NX))
        if k == 0:
            lax.fori_loop(0, NZ, turn, 0)
        settle(x_sem.at[k], halves.at[0:3])
        full[mine, :] = (halves[0] + halves[1]) + (halves[2] + halves[3])
        send(full.at[mine], full.at[mine], s_back.at[k], back_sem.at[k], partner)
        if k == ROUNDS - 1:
            spread_halves(mine)
        settle(back_sem.at[k], full.at[mine])

    def spread_halves(mine):
        k = ROUNDS - 1
        half = loads_in[k, mine, :]
        beta = half[:, COLS : COLS + 1] / loads_in[k - 1, mine, COLS : COLS + 1]
        loads = half[:, 0:COLS] + beta * dir_loads[mine, :]
        norm = jnp.sum(lanes_summed(loads * loads), axis=1, keepdims=True)
        place = lax.broadcasted_iota(jnp.int32, (16, 128), 0) + 16 * core
        here = place == lax.broadcasted_iota(jnp.int32, (16, 128), 1)
        at = core * PEERS + snp
        last[at] = jnp.sum(jnp.where(here, norm, 0.0), axis=0, keepdims=True)
        slot = last.at[at]
        for dz in (4, 3, 5, 2, 6, 1, 7, 0):
            for dy in (2, 1, 3, 0):
                peer = (y + dy) % NY * NZ + (z + dz) % NZ
                if dy or dz:
                    send(slot, slot, s_sc.at[k], sc_sem.at[k], (samp, peer))
                send(slot, slot, s_sc.at[k], sc_sem.at[k], (x * 2 + 1 - core, peer))

    def spread_norms(k):
        loads = dir_loads[...]
        norm = jnp.sum(lanes_summed(loads * loads), axis=1, keepdims=True)
        row = jnp.sum(jnp.where(eye, norm, 0.0), axis=0, keepdims=True)
        scalars[k, snp] = row

        slot = scalars.at[k, snp]
        for dz in (4, 3, 5, 2, 6, 1, 7, 0):
            for dy in (2, 1, 3, 0):
                if dy or dz:
                    other = (samp, (y + dy) % NY * NZ + (z + dz) % NZ)
                    send(slot, slot, s_sc.at[k], sc_sem.at[k], other)

    def total_norms(k):
        if k == ROUNDS - 1:
            settle(sc_sem.at[k], last.at[0 : 2 * PEERS - 1])
            row = jnp.sum(last[...], axis=0)
        else:
            settle(sc_sem.at[k], scalars.at[k, 0 : PEERS - 1])
            row = jnp.sum(scalars[k], axis=0)
        return jnp.sum(jnp.where(eye, row, 0.0), axis=1, keepdims=True)

    def to_image(k):
        image, from_y, to_z, from_z = (
            (u_0, from_y_0, to_z_0, from_z_0), (u_1, from_y_1, to_z_1, from_z_1)
        )[k]
        high, low = split(dir_loads[...] / spread_ref[...])
        lhs[0:ROWS] = high
        lhs[ROWS : 2 * ROWS] = low
        shift = (high.astype(f32) + low.astype(f32)) * centre_ref[...]
        shift = jnp.sum(lanes_summed(shift), axis=1, keepdims=True)

        def multiply(offset):
            zz = (z + offset) % NZ
            both = jnp.dot(lhs[...], turned[:, cols_of(zz)], preferred_element_type=f32)
            image[:, cols_of(zz)] = both[0:ROWS] + both[ROWS : 2 * ROWS] - shift

        def along_y(zz):
            for dy in (2, 1, 3):
                other = (y + dy) % NY
                send(
                    image.at[rows_of(other), cols_of(zz)], from_y.at[dy - 1, :, cols_of(zz)],
                    s_ry.at[k], ry.at[k, zz], at_y(other),
                )

        def chunk(step, carry):
            offset = scatter_order(step)
            multiply(offset)
            zz = (z + offset) % NZ
            beside = (offset == 1) | (offset == 7)

            @pl.when(beside)
            def _():
                send(
                    image.at[:, cols_of(zz)], from_side.at[k, offset // 4],
                    s_rn.at[k], rn.at[k], at_z(zz),
                )

            @pl.when((offset != 0) & ~beside)
            def _():
                along_y(zz)

            return carry

        lax.fori_loop(0, NZ, chunk, 0)
        spread_norms(k)

        def of_y(zz):
            settle(ry.at[k, zz], pieces)
            total = image[rows_of(y), cols_of(zz)]
            for dy in range(NY - 1):
                total = total + from_y[dy, :, cols_of(zz)]
            return total

        def pass_on(offset):
            zz = (z + offset) % NZ
            to_z[zz] = of_y(zz)
            send(to_z.at[zz], from_z.at[offset - 2], s_rz.at[k], rz.at[k], at_z(zz))

        for offset in (4, 3, 5):
            pass_on(offset)
        settle(rn.at[k], from_side.at[k])
        image[:, cols_of(z)] += from_side[k, 0] + from_side[k, 1]
        along_y(z)
        for offset in (2, 6):
            pass_on(offset)
        total = of_y(z)
        settle(rz.at[k], from_z)
        for slot in range(NZ - 3):
            total = total + from_z[slot]
        return total

    norms, squares = [], []
    for k in range(ROUNDS):
        gather(k)
        if k == 0:
            settle(geno_sem, geno)
        to_loads(k)
        over_samp(k)
        loads = loads_in[k, :, 0:COLS]
        norm = loads_in[k, :, COLS : COLS + 1]
        if k == 0:
            dir_loads[...] = loads
            square = norm
        else:
            beta = norm / norms[-1]
            dir_loads[...] = loads + beta * dir_loads[...]
            cross = loads_in[k, :, COLS + 1 : COLS + 2]
            if k == 2:
                cross = cross + betas[0][:, 0:1] * loads_in[k, :, COLS + 2 : COLS + 3]
            square = norm + 2.0 * beta * cross + beta * beta * squares[-1]
            betas[k - 1] = jnp.broadcast_to(beta, (ROWS, 128))
        norms.append(norm)
        squares.append(square)
        if k < ROUNDS - 1:
            summed = to_image(k)
        size = norm / (total_norms(k) * (1.0 / MARKERS) + RIDGE * square)
        steps[k] = jnp.broadcast_to(size, (ROWS, 128))
        gain = size * (1.0 / math.sqrt(SAMPLES))
        if k == 0:
            stats_ref[...] = gain * dir_loads[...]
        else:
            stats_ref[...] += gain * dir_loads[...]
        if k < ROUNDS - 1:
            mine = (rows_of(y), cols_of(z))
            direction = residuals[k][mine]
            if k == 1:
                direction = direction + betas[0, rows_of(y), 0:1] * r_0[mine]
            moved = summed * (1.0 / MARKERS) + RIDGE * direction
            residuals[k + 1][mine] = residuals[k][mine] - steps[k, rows_of(y), 0:1] * moved

    def combined(columns):
        first = r_0[:, columns]
        second = r_1[:, columns] + betas[0][:, 0:1] * first
        third = r_2[:, columns] + betas[1][:, 0:1] * second
        return steps[0][:, 0:1] * first + steps[1][:, 0:1] * second + steps[2][:, 0:1] * third

    solution_ref[:, 0:128] = combined(main_cols(y, z))
    tail = combined(pl.ds(pl.multiple_of(z * CHUNK + 512, 128), 128))
    for yy in range(NY):

        @pl.when(y == yy)
        def _():
            solution_ref[:, 128:160] = tail[:, 32 * yy : 32 * yy + 32]

    for k in range(ROUNDS):
        settle(s_gz.at[k], r_0.at[0:8, 0 : 7 * CHUNK])
        settle(s_gy.at[k], r_0.at[0:24, 0 : 6 * CHUNK])
        settle(s_gn.at[k], r_0.at[0:24, 0 : 2 * CHUNK])
        settle(s_core.at[k], from_core.at[k])
        settle(s_x.at[k], by_x.at[k, 0:3])
        settle(s_back.at[k], from_core.at[k])
    settle(s_sc.at[ROUNDS - 1], last.at[0 : 2 * PEERS - 1])
    for k in range(ROUNDS - 1):
        settle(s_sc.at[k], scalars.at[k, 0 : PEERS - 1])
        settle(s_ry.at[k], r_0.at[0:24, 0 : 6 * CHUNK])
        settle(s_rn.at[k], from_side.at[k])
        settle(s_rz.at[k], from_z_0)


def local(genotype, centre, spread, pheno_probes):
    block = (ROWS, BLOCK)
    dma = pltpu.SemaphoreType.DMA
    vmem = pl.BlockSpec(memory_space=pltpu.VMEM)
    return pl.pallas_call(
        kernel,
        out_shape=(
            jax.ShapeDtypeStruct((ROWS, 160), f32),
            jax.ShapeDtypeStruct((ROWS, COLS), f32),
        ),
        in_specs=[pl.BlockSpec(memory_space=pl.ANY)] * 4,
        out_specs=(vmem, vmem),
        scratch_shapes=[
            pltpu.VMEM((BLOCK, COLS), jnp.bfloat16),
            pltpu.VMEM(block, f32),
            pltpu.VMEM(block, f32),
            pltpu.VMEM(block, f32),
            pltpu.VMEM((NY, NZ, 8, 128), f32),
            pltpu.VMEM(block, f32),
            pltpu.VMEM(block, f32),
            pltpu.VMEM((NY - 1, 8, BLOCK), f32),
            pltpu.VMEM((NY - 1, 8, BLOCK), f32),
            pltpu.VMEM((NZ, 8, CHUNK), f32),
            pltpu.VMEM((NZ, 8, CHUNK), f32),
            pltpu.VMEM((NZ - 3, 8, CHUNK), f32),
            pltpu.VMEM((NZ - 3, 8, CHUNK), f32),
            pltpu.VMEM((2 * ROWS, COLS), f32),
            pltpu.VMEM((4, ROWS, 128), f32),
            pltpu.VMEM((ROUNDS, ROWS, WIDE), f32),
            pltpu.VMEM((ROUNDS, 16, WIDE), f32),
            pltpu.VMEM((ROUNDS, NX, 16, WIDE), f32),
            pltpu.VMEM((ROUNDS, ROWS, WIDE), f32),
            pltpu.VMEM((ROUNDS - 1, PEERS, 1, 128), f32),
            pltpu.VMEM((2 * ROWS, COLS), jnp.bfloat16),
            pltpu.VMEM((ROWS, COLS), f32),
            pltpu.VMEM((ROUNDS, ROWS, 128), f32),
            pltpu.VMEM((ROUNDS - 1, ROWS, 128), f32),
            pltpu.VMEM((2 * PEERS, 1, 128), f32),
            pltpu.VMEM((ROUNDS - 1, 2, ROWS, CHUNK), f32),
            pltpu.VMEM((COLS, BLOCK), jnp.bfloat16),
            pltpu.VMEM((ROWS, 160), f32),
            pltpu.VMEM((1, COLS), f32),
            pltpu.VMEM((1, COLS), f32),
            dma((3,)),
            dma,
            dma((ROUNDS,)),
            dma((ROUNDS,)),
            dma((ROUNDS,)),
            dma((ROUNDS - 1,)),
            dma((ROUNDS - 1,)),
            dma((ROUNDS - 1,)),
            dma((ROUNDS,)),
            dma((ROUNDS,)),
            dma((ROUNDS,)),
            dma((ROUNDS,)),
            dma((ROUNDS, NZ - 1)),
            dma((ROUNDS, NZ)),
            dma((ROUNDS - 1, NZ)),
            dma((ROUNDS - 1,)),
            dma((ROUNDS - 1,)),
            dma((ROUNDS,)),
            dma((ROUNDS,)),
            dma((ROUNDS,)),
            dma((ROUNDS,)),
        ],
        compiler_params=pltpu.CompilerParams(
            collective_id=0, has_side_effects=True, vmem_limit_bytes=60 * 1024 * 1024
        ),
        name="conjugate_gradients",
    )(genotype, pheno_probes, centre, spread)


def solution(mesh):
    in_specs = (P("samp", "snp"), P("snp"), P("snp"), P(None, ("samp", "snp")))
    out_specs = (P(None, ("samp", "snp")), P(None, "snp"))
    return jax.shard_map(local, mesh=mesh, in_specs=in_specs, out_specs=out_specs, check_vma=False)
```

```python
import math

import jax
import jax.numpy as jnp
from jax import lax
from jax.experimental import pallas as pl
from jax.experimental.pallas import tpu as pltpu
from jax.sharding import PartitionSpec as P

SAMPLES = 40960
MARKERS = 40960
ROUNDS = 3
RIDGE = 0.1

ROWS = 32
NY, NZ = 4, 8
NX = 4
PEERS = NY * NZ
CHUNK = 640
BLOCK = CHUNK * NZ
COLS = 1280
WIDE = COLS + 128
PIECE = 8 * CHUNK

MESH = pl.DeviceIdType.MESH
FAR = (2, 6, 3, 5, 4)
SCATTER = (4, 3, 5, 1, 7, 2, 6, 0)
f32 = jnp.float32


def near(step):
    half = (step + 1) // 2
    return jnp.where(step % 2 == 1, half, (NZ - half) % NZ)


def scatter_order(step):
    offset = jnp.int32(SCATTER[0])
    for place in range(1, NZ):
        offset = jnp.where(step == place, SCATTER[place], offset)
    return offset


def split(value):
    high = value.astype(jnp.bfloat16)
    rest = value - high.astype(f32)
    return high, rest.astype(jnp.bfloat16)


def lanes_summed(value):
    total = value[:, 0:128]
    for tile in range(1, value.shape[1] // 128):
        total = total + value[:, 128 * tile : 128 * (tile + 1)]
    return total


def kernel(
    geno_hbm, rhs_hbm, centre_hbm, spread_hbm, solution_ref, stats_ref,
    geno, r_0, r_1, r_2, packed, u_0, u_1, from_y_0, from_y_1, to_z_0, to_z_1,
    from_z_0, from_z_1, partial, acc, loads_out, from_core, by_x, loads_in,
    scalars, lhs, dir_loads, steps, betas,
    last, from_side, turned, rhs_ref, centre_ref, spread_ref, small_sem, geno_sem, s_gz, s_gy, s_gn, s_ry, s_rn, s_rz, s_core, s_x, s_back, s_sc,
    gz, gy, ry, rn, rz, core_sem, x_sem, back_sem, sc_sem,
):
    samp, snp = lax.axis_index("samp"), lax.axis_index("snp")
    x, core = samp // 2, samp % 2
    y, z = snp // NZ, snp % NZ
    residuals = (r_0, r_1, r_2)

    def at_z(other):
        return (samp, y * NZ + other)

    def at_y(other):
        return (samp, other * NZ + z)

    def at_x(other):
        return (other * 2 + core, snp)

    partner = (x * 2 + 1 - core, snp)

    def send(source, target, send_sem, recv_sem, device):
        pltpu.make_async_remote_copy(
            source, target, send_sem, recv_sem, device_id=device, device_id_type=MESH
        ).start()

    def settle(sem, like):
        pltpu.make_async_copy(like, like, sem).wait()

    piece = r_0.at[0:8, 0:CHUNK]
    pieces = r_0.at[0:24, 0:CHUNK]

    def rows_of(group):
        return pl.ds(pl.multiple_of(group * 8, 8), 8)

    def cols_of(chunk):
        return pl.ds(pl.multiple_of(chunk * CHUNK, 128), CHUNK)

    barrier = pltpu.get_barrier_semaphore()

    greeted = [at_z((z + d) % NZ) for d in (4, 3, 5, 2, 6)]
    greeted += [at_y((y + dy) % NY) for dy in (2, 1, 3)]
    greeted += [at_x((x + dx) % NX) for dx in (2, 1, 3)]
    greeted += [at_z((z + d) % NZ) for d in (1, 7)] + [partner]
    for other in greeted:
        pl.semaphore_signal(barrier, inc=1, device_id=other, device_id_type=MESH)
    small = (
        (rhs_hbm, rhs_ref), (centre_hbm, centre_ref.at[0]), (spread_hbm, spread_ref.at[0])
    )
    for which, (source, target) in enumerate(small):
        pltpu.make_async_copy(source, target, small_sem.at[which]).start()

    def main_cols(yy, zz):
        return pl.ds(pl.multiple_of(zz * CHUNK + yy * 128, 128), 128)

    for which, (source, target) in enumerate(small):
        pltpu.make_async_copy(source, target, small_sem.at[which]).wait()
    r_0[:, main_cols(y, z)] = rhs_ref[:, 0:128]
    tails = [rhs_ref[8 * group : 8 * group + 8, 128:160] for group in range(4)]
    packed[y, z] = jnp.concatenate(tails, axis=1)
    for zz in range(NZ):
        for yy in range(NY):
            first = 160 * (yy * NZ + zz)
            pltpu.make_async_copy(
                geno_hbm.at[pl.ds(first, 128)], geno.at[pl.ds(CHUNK * zz + 128 * yy, 128)], geno_sem
            ).start()
            pltpu.make_async_copy(
                geno_hbm.at[pl.ds(first + 128, 32)],
                geno.at[pl.ds(CHUNK * zz + 512 + 32 * yy, 32)],
                geno_sem,
            ).start()

    pl.semaphore_wait(barrier, len(greeted))

    def send_piece(k, yy, zz, send_sem, recv_sem, device):
        if k == 0:
            block = r_0.at[:, main_cols(yy, zz)]
            send(block, block, send_sem, recv_sem, device)
            send(packed.at[yy, zz], packed.at[yy, zz], send_sem, recv_sem, device)
        else:
            block = residuals[k].at[rows_of(yy), cols_of(zz)]
            send(block, block, send_sem, recv_sem, device)

    def forward(k, zz):
        for dy in (2, 1, 3):
            send_piece(k, y, zz, s_gy.at[k], gy.at[k, zz], at_y((y + dy) % NY))

    def pass_forward(k, d):
        settle(gz.at[k, d - 1], piece)
        forward(k, (z - d + NZ) % NZ)

    def gather(k):
        forward(k, z)
        for d in FAR + (1, 7):
            send_piece(k, y, z, s_gz.at[k], gz.at[k, d - 1], at_z((z + d) % NZ))
        settle(gy.at[k, z], pieces)
        for dy in range(1, NY):
            for d in (1, 7):
                other = at_z((z + d) % NZ)
                send_piece(k, (y + dy) % NY, z, s_gn.at[k], gy.at[k, z], other)
        partial[...] = jnp.zeros_like(partial)
        acc[...] = jnp.zeros_like(acc)
        for d in FAR[:2]:
            pass_forward(k, d)

    lane = lax.broadcasted_iota(jnp.int32, (8, 128), 1)

    def unpack(zz):
        sources = [packed[yy, zz] for yy in range(NY)]
        for group in range(4):
            tile = jnp.zeros((8, 128), f32)
            for yy in range(NY):
                shift = (32 * (yy - group)) % 128
                moved = pltpu.roll(sources[yy], shift, 1) if shift else sources[yy]
                tile = jnp.where(lane // 32 == yy, moved, tile)
            start = pl.multiple_of(zz * CHUNK + 512, 128)
            r_0[8 * group : 8 * group + 8, pl.ds(start, 128)] = tile

    def multiply_in(k, zz):
        if k == 0:
            unpack(zz)
        value = residuals[k][:, cols_of(zz)]
        high, low = split(value)
        partial[...] += jnp.dot(
            jnp.concatenate([high, low], axis=0), geno[cols_of(zz), :], preferred_element_type=f32
        )
        acc[0] += lanes_summed(high.astype(f32) + low.astype(f32))
        acc[1] += lanes_summed(value * value)
        if k > 0:
            acc[2] += lanes_summed(value * residuals[k - 1][:, cols_of(zz)])
        if k > 1:
            acc[3] += lanes_summed(value * r_0[:, cols_of(zz)])

    def to_loads(k):
        def chunk(step, carry):
            zz = (z - near(step) + NZ) % NZ

            @pl.when(step > 0)
            def _():
                settle(gy.at[k, zz], pieces)

            multiply_in(k, zz)

            @pl.when(step == 0)
            def _():
                for d in FAR[2:]:
                    pass_forward(k, d)
                for d in (1, 7):
                    settle(gz.at[k, d - 1], piece)

            return carry

        lax.fori_loop(0, NZ, chunk, 0)

    lane32 = lax.broadcasted_iota(jnp.int32, (ROWS, 128), 1)
    eye = lax.broadcasted_iota(jnp.int32, (ROWS, 128), 0) == lane32

    def turn(zz, carry):
        for first in range(0, COLS, 256):
            turned[first : first + 256, cols_of(zz)] = geno[cols_of(zz), first : first + 256].T
        return carry

    def over_samp(k):
        out, got, halves, full = loads_out.at[k], from_core.at[k], by_x.at[k], loads_in.at[k]
        total = jnp.sum(acc[0], axis=1, keepdims=True)
        raw = partial[0:ROWS] + partial[ROWS : 2 * ROWS]
        out[:, 0:COLS] = (raw - total * centre_ref[...]) / spread_ref[...]
        tile = jnp.zeros((ROWS, 128), f32)
        for which in range(1, 2 + k):
            tile = jnp.where(lane32 == which - 1, jnp.sum(acc[which], axis=1, keepdims=True), tile)
        out[:, COLS:WIDE] = tile
        mine = pl.ds(pl.multiple_of(core * 16, 16), 16)
        theirs = pl.ds(pl.multiple_of(16 - core * 16, 16), 16)
        send(out.at[theirs], got, s_core.at[k], core_sem.at[k], partner)
        settle(core_sem.at[k], got)
        halves[x] = out[mine, :] + got[...]
        for dx in (2, 1, 3):
            send(halves.at[x], halves.at[x], s_x.at[k], x_sem.at[k], at_x((x + dx) % NX))
        if k == 0:
            lax.fori_loop(0, NZ, turn, 0)
        settle(x_sem.at[k], halves.at[0:3])
        full[mine, :] = (halves[0] + halves[1]) + (halves[2] + halves[3])
        send(full.at[mine], full.at[mine], s_back.at[k], back_sem.at[k], partner)
        if k == ROUNDS - 1:
            spread_halves(mine)
        settle(back_sem.at[k], full.at[mine])

    def spread_halves(mine):
        k = ROUNDS - 1
        half = loads_in[k, mine, :]
        beta = half[:, COLS : COLS + 1] / loads_in[k - 1, mine, COLS : COLS + 1]
        loads = half[:, 0:COLS] + beta * dir_loads[mine, :]
        norm = jnp.sum(lanes_summed(loads * loads), axis=1, keepdims=True)
        place = lax.broadcasted_iota(jnp.int32, (16, 128), 0) + 16 * core
        here = place == lax.broadcasted_iota(jnp.int32, (16, 128), 1)
        at = core * PEERS + snp
        last[at] = jnp.sum(jnp.where(here, norm, 0.0), axis=0, keepdims=True)
        slot = last.at[at]
        for dz in (4, 3, 5, 2, 6, 1, 7, 0):
            for dy in (2, 1, 3, 0):
                peer = (y + dy) % NY * NZ + (z + dz) % NZ
                if dy or dz:
                    send(slot, slot, s_sc.at[k], sc_sem.at[k], (samp, peer))
                send(slot, slot, s_sc.at[k], sc_sem.at[k], (x * 2 + 1 - core, peer))

    def spread_norms(k):
        loads = dir_loads[...]
        norm = jnp.sum(lanes_summed(loads * loads), axis=1, keepdims=True)
        row = jnp.sum(jnp.where(eye, norm, 0.0), axis=0, keepdims=True)
        scalars[k, snp] = row

        slot = scalars.at[k, snp]
        for dz in (4, 3, 5, 2, 6, 1, 7, 0):
            for dy in (2, 1, 3, 0):
                if dy or dz:
                    other = (samp, (y + dy) % NY * NZ + (z + dz) % NZ)
                    send(slot, slot, s_sc.at[k], sc_sem.at[k], other)

    def total_norms(k):
        if k == ROUNDS - 1:
            settle(sc_sem.at[k], last.at[0 : 2 * PEERS - 1])
            row = jnp.sum(last[...], axis=0)
        else:
            settle(sc_sem.at[k], scalars.at[k, 0 : PEERS - 1])
            row = jnp.sum(scalars[k], axis=0)
        return jnp.sum(jnp.where(eye, row, 0.0), axis=1, keepdims=True)

    def to_image(k):
        image, from_y, to_z, from_z = (
            (u_0, from_y_0, to_z_0, from_z_0), (u_1, from_y_1, to_z_1, from_z_1)
        )[k]
        high, low = split(dir_loads[...] / spread_ref[...])
        lhs[0:ROWS] = high
        lhs[ROWS : 2 * ROWS] = low
        shift = (high.astype(f32) + low.astype(f32)) * centre_ref[...]
        shift = jnp.sum(lanes_summed(shift), axis=1, keepdims=True)

        def multiply(offset):
            zz = (z + offset) % NZ
            both = jnp.dot(lhs[...], turned[:, cols_of(zz)], preferred_element_type=f32)
            image[:, cols_of(zz)] = both[0:ROWS] + both[ROWS : 2 * ROWS] - shift

        def along_y(zz):
            for dy in (2, 1, 3):
                other = (y + dy) % NY
                send(
                    image.at[rows_of(other), cols_of(zz)], from_y.at[dy - 1, :, cols_of(zz)],
                    s_ry.at[k], ry.at[k, zz], at_y(other),
                )

        def chunk(step, carry):
            offset = scatter_order(step)
            multiply(offset)
            zz = (z + offset) % NZ
            beside = (offset == 1) | (offset == 7)

            @pl.when(beside)
            def _():
                send(
                    image.at[:, cols_of(zz)], from_side.at[k, offset // 4],
                    s_rn.at[k], rn.at[k], at_z(zz),
                )

            @pl.when((offset != 0) & ~beside)
            def _():
                along_y(zz)

            return carry

        lax.fori_loop(0, NZ, chunk, 0)
        spread_norms(k)

        def of_y(zz):
            settle(ry.at[k, zz], pieces)
            total = image[rows_of(y), cols_of(zz)]
            for dy in range(NY - 1):
                total = total + from_y[dy, :, cols_of(zz)]
            return total

        def pass_on(offset):
            zz = (z + offset) % NZ
            to_z[zz] = of_y(zz)
            send(to_z.at[zz], from_z.at[offset - 2], s_rz.at[k], rz.at[k], at_z(zz))

        for offset in (4, 3, 5, 2):
            pass_on(offset)
        settle(rn.at[k], from_side.at[k])
        image[:, cols_of(z)] += from_side[k, 0] + from_side[k, 1]
        along_y(z)
        for offset in (6,):
            pass_on(offset)
        total = of_y(z)
        settle(rz.at[k], from_z)
        for slot in range(NZ - 3):
            total = total + from_z[slot]
        return total

    norms, squares = [], []
    for k in range(ROUNDS):
        gather(k)
        if k == 0:
            settle(geno_sem, geno)
        to_loads(k)
        over_samp(k)
        loads = loads_in[k, :, 0:COLS]
        norm = loads_in[k, :, COLS : COLS + 1]
        if k == 0:
            dir_loads[...] = loads
            square = norm
        else:
            beta = norm / norms[-1]
            dir_loads[...] = loads + beta * dir_loads[...]
            cross = loads_in[k, :, COLS + 1 : COLS + 2]
            if k == 2:
                cross = cross + betas[0][:, 0:1] * loads_in[k, :, COLS + 2 : COLS + 3]
            square = norm + 2.0 * beta * cross + beta * beta * squares[-1]
            betas[k - 1] = jnp.broadcast_to(beta, (ROWS, 128))
        norms.append(norm)
        squares.append(square)
        if k < ROUNDS - 1:
            summed = to_image(k)
        size = norm / (total_norms(k) * (1.0 / MARKERS) + RIDGE * square)
        steps[k] = jnp.broadcast_to(size, (ROWS, 128))
        gain = size * (1.0 / math.sqrt(SAMPLES))
        if k == 0:
            stats_ref[...] = gain * dir_loads[...]
        else:
            stats_ref[...] += gain * dir_loads[...]
        if k < ROUNDS - 1:
            mine = (rows_of(y), cols_of(z))
            direction = residuals[k][mine]
            if k == 1:
                direction = direction + betas[0, rows_of(y), 0:1] * r_0[mine]
            moved = summed * (1.0 / MARKERS) + RIDGE * direction
            residuals[k + 1][mine] = residuals[k][mine] - steps[k, rows_of(y), 0:1] * moved

    def combined(columns):
        first = r_0[:, columns]
        second = r_1[:, columns] + betas[0][:, 0:1] * first
        third = r_2[:, columns] + betas[1][:, 0:1] * second
        return steps[0][:, 0:1] * first + steps[1][:, 0:1] * second + steps[2][:, 0:1] * third

    solution_ref[:, 0:128] = combined(main_cols(y, z))
    tail = combined(pl.ds(pl.multiple_of(z * CHUNK + 512, 128), 128))
    for yy in range(NY):

        @pl.when(y == yy)
        def _():
            solution_ref[:, 128:160] = tail[:, 32 * yy : 32 * yy + 32]

    for k in range(ROUNDS):
        settle(s_gz.at[k], r_0.at[0:8, 0 : 7 * CHUNK])
        settle(s_gy.at[k], r_0.at[0:24, 0 : 6 * CHUNK])
        settle(s_gn.at[k], r_0.at[0:24, 0 : 2 * CHUNK])
        settle(s_core.at[k], from_core.at[k])
        settle(s_x.at[k], by_x.at[k, 0:3])
        settle(s_back.at[k], from_core.at[k])
    settle(s_sc.at[ROUNDS - 1], last.at[0 : 2 * PEERS - 1])
    for k in range(ROUNDS - 1):
        settle(s_sc.at[k], scalars.at[k, 0 : PEERS - 1])
        settle(s_ry.at[k], r_0.at[0:24, 0 : 6 * CHUNK])
        settle(s_rn.at[k], from_side.at[k])
        settle(s_rz.at[k], from_z_0)


def local(genotype, centre, spread, pheno_probes):
    block = (ROWS, BLOCK)
    dma = pltpu.SemaphoreType.DMA
    vmem = pl.BlockSpec(memory_space=pltpu.VMEM)
    return pl.pallas_call(
        kernel,
        out_shape=(
            jax.ShapeDtypeStruct((ROWS, 160), f32),
            jax.ShapeDtypeStruct((ROWS, COLS), f32),
        ),
        in_specs=[pl.BlockSpec(memory_space=pl.ANY)] * 4,
        out_specs=(vmem, vmem),
        scratch_shapes=[
            pltpu.VMEM((BLOCK, COLS), jnp.bfloat16),
            pltpu.VMEM(block, f32),
            pltpu.VMEM(block, f32),
            pltpu.VMEM(block, f32),
            pltpu.VMEM((NY, NZ, 8, 128), f32),
            pltpu.VMEM(block, f32),
            pltpu.VMEM(block, f32),
            pltpu.VMEM((NY - 1, 8, BLOCK), f32),
            pltpu.VMEM((NY - 1, 8, BLOCK), f32),
            pltpu.VMEM((NZ, 8, CHUNK), f32),
            pltpu.VMEM((NZ, 8, CHUNK), f32),
            pltpu.VMEM((NZ - 3, 8, CHUNK), f32),
            pltpu.VMEM((NZ - 3, 8, CHUNK), f32),
            pltpu.VMEM((2 * ROWS, COLS), f32),
            pltpu.VMEM((4, ROWS, 128), f32),
            pltpu.VMEM((ROUNDS, ROWS, WIDE), f32),
            pltpu.VMEM((ROUNDS, 16, WIDE), f32),
            pltpu.VMEM((ROUNDS, NX, 16, WIDE), f32),
            pltpu.VMEM((ROUNDS, ROWS, WIDE), f32),
            pltpu.VMEM((ROUNDS - 1, PEERS, 1, 128), f32),
            pltpu.VMEM((2 * ROWS, COLS), jnp.bfloat16),
            pltpu.VMEM((ROWS, COLS), f32),
            pltpu.VMEM((ROUNDS, ROWS, 128), f32),
            pltpu.VMEM((ROUNDS - 1, ROWS, 128), f32),
            pltpu.VMEM((2 * PEERS, 1, 128), f32),
            pltpu.VMEM((ROUNDS - 1, 2, ROWS, CHUNK), f32),
            pltpu.VMEM((COLS, BLOCK), jnp.bfloat16),
            pltpu.VMEM((ROWS, 160), f32),
            pltpu.VMEM((1, COLS), f32),
            pltpu.VMEM((1, COLS), f32),
            dma((3,)),
            dma,
            dma((ROUNDS,)),
            dma((ROUNDS,)),
            dma((ROUNDS,)),
            dma((ROUNDS - 1,)),
            dma((ROUNDS - 1,)),
            dma((ROUNDS - 1,)),
            dma((ROUNDS,)),
            dma((ROUNDS,)),
            dma((ROUNDS,)),
            dma((ROUNDS,)),
            dma((ROUNDS, NZ - 1)),
            dma((ROUNDS, NZ)),
            dma((ROUNDS - 1, NZ)),
            dma((ROUNDS - 1,)),
            dma((ROUNDS - 1,)),
            dma((ROUNDS,)),
            dma((ROUNDS,)),
            dma((ROUNDS,)),
            dma((ROUNDS,)),
        ],
        compiler_params=pltpu.CompilerParams(
            collective_id=0, has_side_effects=True, vmem_limit_bytes=60 * 1024 * 1024
        ),
        name="conjugate_gradients",
    )(genotype, pheno_probes, centre, spread)


def solution(mesh):
    in_specs = (P("samp", "snp"), P("snp"), P("snp"), P(None, ("samp", "snp")))
    out_specs = (P(None, ("samp", "snp")), P(None, "snp"))
    return jax.shard_map(local, mesh=mesh, in_specs=in_specs, out_specs=out_specs, check_vma=False)
```
